32 devices in a mesh: member: 2 (over core), tile: 16 (over z, y, x).
Axes of the slice: x: 2, y: 2, z: 4, core: 2. Of those that a mesh axis runs over, the one named last changes fastest.
Arguments:
- ensemble: bfloat16 [40, 7, 32, 2048], P('member', None, None, 'tile'), may hold values from -6 to 6
- control: bfloat16 [40, 32, 2048], P('member', None, 'tile'), may hold values from -6 to 6
- vert_loc: bfloat16 [32, 32], replicated, may hold values from -1 to 1
- obs_source: int32 [8192, 1], P('tile'), may hold values from 0 to 15; in each aligned block of 512 rows (0 to 511, 512 to 1023, ...) at most 64 rows name the same one
- obs_column: int32 [8192], P('tile'), may hold values from 0 to 127
- obs_slot: int32 [8192], P('tile'), may hold values from 0 to 5
- obs_frac: float32 [8192], P('tile'), may hold values from 0 to 1
- obs_count: int32 [16], P('tile'), may hold values from 1 to 512, 4096 in all
Outputs:
- obs_increment: float32 [32, 8192], P(None, 'tile')
The draws below stay inside these ranges and needn't reach their ends.
Inputs may be any that keep to these rules, and one draw needn't show every extreme that they name: `obs_source`: among the 512 observation slots of one owner tile, at most 64 name the same source tile, and some source tile is named exactly 64 times. `obs_count`: the counts sum to 4096 and one of them is 512.
All inputs are finite; a program needn't handle non-finite values. No bound on the sum of `obs_count` on one device may be relied on, other than what follows from the above.
Results may differ from the reference program's by a relative error of at most 0.0003.
Values sent between devices are 32-bit elements; how exact they have to be, the bound alone decides.
A program may use at most 64 MiB of HBM per device.

```python
import math
import jax
import jax.numpy as jnp
import numpy as np
from jax import lax

MEM = 40
SLOTS = 7
LEV = 32
COL_DEV = 128
OBS_DEV = 512
COLS = 2048
OBS = 8192
CAP = 64
N_TILE = 16


def set_ends(result, own_key, low, largest):
    place = [jax.random.randint(jax.random.fold_in(own_key, axis), (), 0, length) for axis, length in enumerate(result.shape)]
    widest = result.shape.index(max(result.shape))
    neighbour = place[:widest] + [(place[widest] + 1) % result.shape[widest]] + place[widest + 1:]
    return result.at[tuple(place)].set(low).at[tuple(neighbour)].set(largest)


def level_of(key, shape, shards, low, largest):
    level = 1.0
    for axis_at, shards_of in shards:
        draws = jax.random.uniform(jax.random.fold_in(jax.random.fold_in(key, 6), axis_at), (shards_of,), jnp.float32, low / len(shards), largest / len(shards))
        level = level * jnp.repeat(jnp.exp(draws), shape[axis_at] // shards_of).reshape((-1,) + (1,) * (len(shape) - 1 - axis_at))
    return level


def split_up(number_of, total, limit, skew):
    portions = [(1 << 20) // math.isqrt(standing ** skew) + 1 for standing in range(2, number_of + 1)]
    spare, given = total - limit - (number_of - 1), [1] * (number_of - 1)
    while spare > 0:
        free = [i for i in range(number_of - 1) if given[i] < limit]
        mass, left = sum([portions[i] for i in free]), spare
        for i in free:
            extra = min(limit - given[i], max(1, left * portions[i] // mass), spare)
            given[i] = given[i] + extra
            spare = spare - extra
    return np.array([limit] + given)


def ragged(rng, count, total, limit, skew):
    if count == 2:
        one = jax.random.randint(rng, (), max(1, total - limit), min(limit, total - 1) + 1)
        return jnp.stack([one, total - one])
    lengths = jnp.asarray(split_up(count, total, limit, skew), jnp.int32)
    couples = (count - 1) // 2
    donor, taker = lengths[1:1 + 2 * couples:2], lengths[2:2 + 2 * couples:2]
    room = jnp.minimum(donor - 1, limit - taker)
    passed = jax.random.randint(jax.random.fold_in(rng, 1), (couples,), 0, 1 << 20) % (room + 1)
    lengths = lengths.at[1:1 + 2 * couples:2].set(donor - passed).at[2:2 + 2 * couples:2].set(taker + passed)
    return lengths[jax.random.permutation(jax.random.fold_in(rng, 2), count)]


def deal_out(rng, own, number, rows, number_of, top, limit, slope):
    order = jax.random.permutation(rng, number_of)
    crowded, common = load_shares(number_of, rows * top, limit, slope, True), load_shares(number_of, rows * top, limit, slope, False)
    places = jnp.arange(number_of)

    def named(sizes, turn):
        used = int((sizes > 0).sum())
        fixed = max(1, used // 4)
        shifted = fixed + (places - fixed + turn * (used - fixed)) % max(1, number_of - fixed)
        return jnp.zeros((number_of,), jnp.int32).at[order[jnp.where(places < fixed, places, shifted)]].set(jnp.asarray(sizes, jnp.int32))

    sizes = jnp.where(number % 4 == 0, named(crowded, number // 4), named(common, number - number // 4 - 1))
    mixed = jax.random.permutation(jax.random.fold_in(own, 3), number_of)
    giver, sink = mixed[0:number_of // 2 * 2:2], mixed[1:number_of // 2 * 2:2]
    slack = jnp.minimum(sizes[giver] - 1, limit - sizes[sink]) // 2
    slack = jnp.where((giver == order[0]) | (sink == order[0]) | (sizes[sink] == 0), 0, jnp.maximum(slack, 0))
    shifted = jax.random.randint(jax.random.fold_in(own, 4), (number_of // 2,), 0, 1 << 20) % (slack + 1)
    sizes = sizes.at[giver].add(-shifted).at[sink].add(shifted)
    items = jnp.searchsorted(jnp.cumsum(sizes), jnp.arange(rows * top), side="right").astype(jnp.int32)
    listing = items.reshape(top, rows).T
    listing = listing[jax.random.permutation(jax.random.fold_in(own, 1), rows)]
    turn = jax.random.randint(jax.random.fold_in(own, 2), (rows, 1), 0, top)
    return jnp.take_along_axis(listing, (jnp.arange(top)[None, :] + turn) % top, axis=1)


def load_shares(amount, total, most, slope, full):
    loads = [(1 << 20) // math.isqrt(standing ** slope) + 1 for standing in range(1, amount + 1)]
    largest = most if full else min(most, max(-(-total // amount), total * loads[0] // sum(loads)))
    least = 1 if total - largest >= amount - 1 else 0
    given, surplus = [largest] + [least] * (amount - 1), total - largest - least * (amount - 1)
    while surplus > 0:
        movable = [i for i in range(1, amount) if given[i] < largest] or [i for i in range(1, amount) if given[i] < most]
        pool, budget = sum([loads[i] for i in movable]), surplus
        for i in movable:
            more = min(most - given[i], max(1, budget * loads[i] // pool), surplus)
            given[i] = given[i] + more
            surplus = surplus - more
    return np.array(given)


def scatter_about(key, shape, scale, reach, pieces=(), held_as=jnp.bfloat16):
    level = level_of(key, shape, pieces, -0.22, 0.18) if pieces else 1.0
    entries = jax.random.normal(key, shape, jnp.float32) * scale * level
    return jnp.minimum(jnp.maximum(entries, -reach), reach).astype(held_as)


def setup_inputs(seed: int = 0) -> dict:
    key_of = jax.random.split(jax.random.key(seed), 9)
    ensemble = scatter_about(key_of[0], (MEM, SLOTS, LEV, COLS), 1.0, 6.0, ((0, 2), (3, 16)))
    control = scatter_about(key_of[1], (MEM, LEV, COLS), 1.0, 6.0, ((0, 2), (2, 16)))
    vert_loc = scatter_about(key_of[2], (LEV, LEV), LEV ** -0.5, 1.0)
    obs_source_keys = jax.random.split(jax.random.fold_in(key_of[3], 1), OBS // OBS_DEV)
    obs_source_turns = jax.random.permutation(jax.random.fold_in(key_of[3], 3), OBS // OBS_DEV)
    obs_source = jax.vmap(lambda own, number: deal_out(jax.random.fold_in(key_of[3], 2), own, number, OBS_DEV, N_TILE, 1, CAP, 2))(obs_source_keys, obs_source_turns).reshape((OBS, 1))
    obs_column = set_ends(jax.random.randint(key_of[4], (OBS,), 0, COL_DEV), jax.random.fold_in(key_of[4], 1), 0, COL_DEV - 1).astype(jnp.int32)
    obs_slot = set_ends(jax.random.randint(key_of[5], (OBS,), 0, SLOTS - 1), jax.random.fold_in(key_of[5], 1), 0, (SLOTS - 1) - 1).astype(jnp.int32)
    obs_frac = jnp.clip(1.0 * jax.random.uniform(key_of[6], (OBS,), jnp.float32) ** level_of(key_of[6], (OBS,), ((0, 16),), -0.2, 0.2), 0.0, 1.0)
    obs_count = ragged(key_of[7], N_TILE, OBS // 2, OBS_DEV, 2).astype(jnp.int32)
    return dict(ensemble=ensemble, control=control, vert_loc=vert_loc, obs_source=obs_source, obs_column=obs_column, obs_slot=obs_slot, obs_frac=obs_frac, obs_count=obs_count)


def reference(ensemble, control, vert_loc, obs_source, obs_column, obs_slot, obs_frac, obs_count):
    loc_float = vert_loc.astype(jnp.float32)

    def member_step(total, pair):
        member, ctrl = pair
        weighted = jnp.dot(loc_float, ctrl.astype(jnp.float32), precision=lax.Precision.HIGHEST)
        return total + member.astype(jnp.float32) * weighted[None], None

    start = jnp.zeros((SLOTS, LEV, COLS), jnp.float32)
    increment, _ = lax.scan(member_step, start, (ensemble, control))
    glob = (obs_source[:, 0] * COL_DEV + obs_column).astype(jnp.int32)
    lower = increment[obs_slot, :, glob].T
    upper = increment[obs_slot + 1, :, glob].T
    frac = obs_frac[None, :]
    value = (1.0 - frac) * lower + frac * upper
    live = (jnp.arange(OBS, dtype=jnp.int32) % OBS_DEV) < jnp.repeat(obs_count, OBS_DEV)
    return jnp.where(live[None, :], value, jnp.float32(0.0))
```

```python
import functools

import jax
import jax.numpy as jnp
from jax import lax
from jax.experimental import pallas as pl
from jax.experimental.pallas import tpu as pltpu
from jax.sharding import PartitionSpec as P

MESH = pl.DeviceIdType.MESH
LANES = 128
F32 = jnp.float32
BF16 = jnp.bfloat16


def iota(shape, axis):
    return lax.broadcasted_iota(jnp.int32, shape, axis)


def one_hot(condition):
    return jnp.where(condition, F32(1.0), F32(0.0)).astype(BF16)


def dot(a, b):
    return jnp.dot(a, b, preferred_element_type=F32)


def dot_nt(a, b):
    return lax.dot_general(a, b, (((1,), (1,)), ((), ())), preferred_element_type=F32)


def two_pieces(x):
    high = x.astype(BF16)
    return high, (x - high.astype(F32)).astype(BF16)


def turned(x, shift):
    shift = shift % LANES
    return x if shift == 0 else pltpu.roll(x, shift, 1)


def kernel(
    tiles, groups, near, cap, packs,
    ens_hbm, ctl_hbm, vloc_hbm, source_hbm, column_hbm, slot_hbm, frac_hbm, count_ref,
    out_ref,
    vloc_ref, source_ref, column_ref, slot_ref, frac_ref, ens, ctl, weighted, part, part_in, asked, relay, req_in, res_out, res_in, place,
    load_sem, part_send, part_recv, near_send, near_recv, far_send, far_recv, res_send, res_recv,
):
    me = lax.axis_index("tile")
    mine = lax.axis_index("member")
    leader = groups - 1
    leads = mine == leader
    members, slots, levels, cols = ens.shape
    rows = levels // packs
    obs = column_ref.shape[1]
    owners = LANES // cap
    far = tiles // near
    low, high = lax.rem(me, near), me // near
    chunk = max(near, owners)
    chunks = tiles // chunk
    lines = chunk // near
    spans = chunk // owners
    width = spans * LANES

    def loaded(index, source, target):
        return pltpu.make_async_copy(source, target, load_sem.at[index])

    loads = [
        loaded(0, source_hbm, source_ref), loaded(1, column_hbm, column_ref),
        loaded(2, slot_hbm, slot_ref), loaded(3, frac_hbm, frac_ref),
        loaded(4, vloc_hbm, vloc_ref), loaded(5, ctl_hbm, ctl), loaded(6, ens_hbm, ens),
    ]

    def near_peer(step):
        return lax.rem(low + step, near)

    def far_peer(step):
        return lax.rem(high + step, far)

    barrier = pltpu.get_barrier_semaphore()

    def greet(tile, member):
        pl.semaphore_signal(
            barrier, inc=1, device_id={"tile": tile, "member": member}, device_id_type=MESH
        )

    @pl.when(leads)
    def _():
        for step in range(1, far):
            greet(far_peer(step) * near + low, leader)
        for step in range(1, near):
            greet(high * near + near_peer(step), leader)
        for member in range(leader):
            greet(me, member)

    @pl.when(jnp.logical_not(leads))
    def _():
        greet(me, leader)

    for load in loads:
        load.start()

    for load in loads[:4]:
        load.wait()
    source = source_ref[...]
    hits = source == iota((tiles, obs), 0)
    hits_f = jnp.where(hits, F32(1.0), F32(0.0))
    before = one_hot(iota((LANES, LANES), 0) < iota((LANES, LANES), 1))
    seen = jnp.zeros((tiles, 1), F32)
    ranks = []
    for block in range(obs // LANES):
        hit = hits_f[:, block * LANES:(block + 1) * LANES]
        ahead = dot(hit.astype(BF16), before) + seen
        ranks.append(jnp.sum(ahead * hit, axis=0, keepdims=True))
        seen = seen + jnp.sum(hit, axis=1, keepdims=True)
    rank = jnp.concatenate(ranks, axis=1).astype(jnp.int32)

    @pl.when(leads)
    def _():
        spread = one_hot(rank == lax.rem(iota((LANES, obs), 0), cap))
        frac = frac_ref[...]
        frac_0 = frac.astype(BF16).astype(F32)
        frac_1 = (frac - frac_0).astype(BF16).astype(F32)
        frac_2 = frac - frac_0 - frac_1
        values = [column_ref[...].astype(F32), slot_ref[...].astype(F32), frac_0, frac_1, frac_2]
        packed = dot_nt(
            jnp.concatenate([jnp.where(hits, v, F32(0.0)) for v in values], axis=0).astype(BF16), spread
        )
        packed = [packed[i * tiles:(i + 1) * tiles] for i in range(len(values))]
        request = jnp.where(
            iota((tiles, LANES), 1) < cap,
            packed[0] + cols * packed[1],
            packed[2] + packed[3] + packed[4],
        )
        for tile in range(tiles):
            asked[tile % near, tile // near] = request[tile:tile + 1]

    batch = max(d for d in range(1, max(1, LANES // levels) + 1) if members % d == 0)
    wide = batch * levels
    repeat = one_hot(lax.rem(iota((wide, levels), 0), levels) == iota((wide, levels), 1))
    for load in loads[4:6]:
        load.wait()
    tall = dot(repeat, vloc_ref[...]).astype(BF16)
    full = dot_nt(tall, repeat)
    factor = jnp.where(
        iota((wide, wide), 0) // levels == iota((wide, wide), 1) // levels, full, F32(0.0)
    ).astype(BF16)
    for step in range(members // batch):
        weighted[step * wide:(step + 1) * wide] = dot(factor, ctl[step * wide:(step + 1) * wide])

    loads[6].wait()
    for slot in range(slots):
        total = jnp.zeros((levels, cols), F32)
        for k in range(members):
            total = total + ens[k, slot].astype(F32) * weighted[k * levels:(k + 1) * levels]
        part[slot * levels:(slot + 1) * levels] = total

    def give(member):
        return pltpu.make_async_remote_copy(
            src_ref=part, dst_ref=part_in.at[member],
            send_sem=part_send, recv_sem=part_recv.at[member],
            device_id={"tile": me, "member": leader}, device_id_type=MESH,
        )

    @pl.when(jnp.logical_not(leads))
    def _():
        pl.semaphore_wait(barrier, 1)
        give(mine).start()

    position = source * cap + rank
    place[...] = one_hot(position == iota((tiles * cap, obs), 0))

    lane = iota((1, LANES), 1)
    stride = jnp.where(2 * me < tiles, 1, chunks - 1)
    home = me // chunk

    def chunk_at(step):
        return lax.rem(home + stride * step, chunks)

    def unless(step, condition, body):
        if step == 0:
            pl.when(condition)(body)
        else:
            body()

    def reply_to(tile, member):
        return pltpu.make_async_remote_copy(
            src_ref=res_out.at[tile], dst_ref=res_in.at[me],
            send_sem=res_send.at[member], recv_sem=res_recv.at[home],
            device_id={"tile": tile, "member": member}, device_id_type=MESH,
        )

    def landed(source, target, send, recv):
        return pltpu.make_async_remote_copy(
            src_ref=source, dst_ref=target, send_sem=send, recv_sem=recv,
            device_id={"tile": me, "member": leader}, device_id_type=MESH,
        )

    @pl.when(leads)
    def _():
        def near_copy(peer, line):
            return pltpu.make_async_remote_copy(
                src_ref=asked.at[peer], dst_ref=relay.at[line],
                send_sem=near_send, recv_sem=near_recv.at[line],
                device_id={"tile": high * near + peer, "member": leader}, device_id_type=MESH,
            )

        def far_copy(peer, line):
            return pltpu.make_async_remote_copy(
                src_ref=relay.at[:, peer], dst_ref=req_in.at[pl.ds(line * near, near)],
                send_sem=far_send, recv_sem=far_recv.at[line],
                device_id={"tile": peer * near + low, "member": leader}, device_id_type=MESH,
            )

        relay[low] = asked[low]
        pl.semaphore_wait(barrier, near + far + groups - 3)
        for step in range(1, near):
            near_copy(near_peer(step), low).start()
        for step in range(1, near):
            near_copy(near_peer(step), near_peer(step)).wait_recv()
        for step in range(1, far):
            far_copy(far_peer(step), high).start()
        req_in[pl.ds(high * near, near)] = relay[:, high]

        increment = part[...]
        for member in range(leader):
            give(member).wait_recv()
            increment = increment + part_in[member]
        pieces = jnp.concatenate(two_pieces(increment), axis=1)

        for step in range(chunks):
            group = chunk_at(step)
            for i in range(lines):
                line = group * lines + i
                unless(step, line != high, lambda line=line: far_copy(line, line).wait_recv())
            codes, fracs = [], []
            for s in range(spans):
                code = jnp.zeros((1, LANES), F32)
                frac = jnp.zeros((1, LANES), F32)
                for i in range(owners):
                    got = req_in[group * chunk + s * owners + i]
                    here = lane // cap == i
                    code = jnp.where(here, turned(got, i * cap), code)
                    frac = jnp.where(here, turned(got, i * cap - cap), frac)
                codes.append(code)
                fracs.append(frac)
            code = jnp.concatenate(codes, axis=1).astype(jnp.int32)
            frac = jnp.concatenate(fracs, axis=1)
            wanted = code // cols
            column = code - wanted * cols
            pick = one_hot(iota((cols, width), 0) == column)
            columns = dot(pieces, jnp.concatenate([pick, pick], axis=0))
            answer = jnp.zeros((levels, width), F32)
            for slot in range(slots):
                weight = jnp.where(
                    wanted == slot, 1.0 - frac, jnp.where(wanted + 1 == slot, frac, F32(0.0))
                )
                answer = answer + weight * columns[slot * levels:(slot + 1) * levels]
            for t in range(chunk):
                s, i = t // owners, t % owners
                tile = group * chunk + t
                packet = jnp.zeros((rows, LANES), F32)
                for j in range(packs):
                    block = answer[j * rows:(j + 1) * rows, s * LANES:(s + 1) * LANES]
                    packet = jnp.where(lane // cap == j, turned(block, (j - i) * cap), packet)
                res_out[tile] = packet
                if step == 0:
                    @pl.when(tile == me)
                    def _():
                        res_in[me] = packet
                unless(step, tile != me, lambda tile=tile: reply_to(tile, leader).start())
                for member in range(leader):
                    reply_to(tile, member).start()

    both = jnp.zeros((2 * levels, obs), F32)
    for step in range(chunks):
        group = chunk_at(step)
        whole = res_in.at[pl.ds(group * chunk, chunk)]
        if step == 0:
            if chunk > 1:
                @pl.when(leads)
                def _():
                    rest = res_in.at[pl.ds(0, chunk - 1)]
                    landed(rest, rest, res_send.at[leader], res_recv.at[group]).wait_recv()

            @pl.when(jnp.logical_not(leads))
            def _():
                landed(whole, whole, res_send.at[leader], res_recv.at[group]).wait_recv()
        else:
            landed(whole, whole, res_send.at[leader], res_recv.at[group]).wait_recv()
        columns = []
        for s in range(spans):
            bands = [jnp.zeros((rows, LANES), F32)] * packs
            for i in range(owners):
                got = res_in[group * chunk + s * owners + i]
                for j in range(packs):
                    bands[j] = jnp.where(lane // cap == i, turned(got, (i - j) * cap), bands[j])
            columns.append(jnp.concatenate(bands, axis=0))
        upper, lower = two_pieces(jnp.concatenate(columns, axis=1))
        first = pl.multiple_of(group * width, LANES)
        both = both + dot(jnp.concatenate([upper, lower], axis=0), place[pl.ds(first, width)])
    live = iota((levels, obs), 1) < count_ref[0]
    out_ref[...] = jnp.where(live, both[:levels] + both[levels:], F32(0.0))

    @pl.when(jnp.logical_not(leads))
    def _():
        give(mine).wait_send()

    @pl.when(leads)
    def _():
        def sent(buffer, sem):
            landed(buffer, buffer, sem, far_recv.at[0]).wait_send()

        if near > 1:
            sent(asked.at[pl.ds(0, near - 1)], near_send)
        if far > 1:
            sent(req_in.at[pl.ds(0, (far - 1) * near)], far_send)
        for member in range(leader):
            sent(res_out, res_send.at[member])
        if tiles > 1:
            sent(res_out.at[pl.ds(0, tiles - 1)], res_send.at[leader])


def on_device(ensemble, control, vert_loc, obs_source, obs_column, obs_slot, obs_frac, obs_count):
    tiles, groups = lax.axis_size("tile"), lax.axis_size("member")
    members, slots, levels, cols = ensemble.shape
    obs = obs_column.shape[0]
    cap = max(4, 2 * obs // tiles)
    near = max(d for d in range(1, tiles + 1) if tiles % d == 0 and d * d <= tiles)
    packs = max(1, min(LANES // cap, levels // 8))
    rows = levels // packs
    chunks = tiles // max(near, LANES // cap)
    vmem = pl.BlockSpec(memory_space=pltpu.VMEM)
    hbm = pl.BlockSpec(memory_space=pl.ANY)
    dma = pltpu.SemaphoreType.DMA
    return pl.pallas_call(
        functools.partial(kernel, tiles, groups, near, cap, packs),
        out_shape=pltpu.VMEM((levels, obs), F32),
        in_specs=[hbm] * 7 + [pl.BlockSpec(memory_space=pltpu.SMEM)],
        out_specs=vmem,
        scratch_shapes=[
            pltpu.VMEM((levels, levels), BF16),
            pltpu.VMEM((1, obs), jnp.int32),
            pltpu.VMEM((1, obs), jnp.int32),
            pltpu.VMEM((1, obs), jnp.int32),
            pltpu.VMEM((1, obs), F32),
            pltpu.VMEM((members, slots, levels, cols), BF16),
            pltpu.VMEM((members * levels, cols), BF16),
            pltpu.VMEM((members * levels, cols), F32),
            pltpu.VMEM((slots * levels, cols), F32),
            pltpu.VMEM((max(1, groups - 1), slots * levels, cols), F32),
            pltpu.VMEM((near, tiles // near, 1, LANES), F32),
            pltpu.VMEM((near, tiles // near, 1, LANES), F32),
            pltpu.VMEM((tiles, 1, LANES), F32),
            pltpu.VMEM((tiles, rows, LANES), F32),
            pltpu.VMEM((tiles, rows, LANES), F32),
            pltpu.VMEM((tiles * cap, obs), BF16),
            dma((7,)),
            dma,
            dma((max(1, groups - 1),)),
            dma,
            dma((near,)),
            dma,
            dma((tiles // near,)),
            dma((groups,)),
            dma((chunks,)),
        ],
        compiler_params=pltpu.CompilerParams(collective_id=0, has_side_effects=True),
    )(
        ensemble,
        control.reshape(members * levels, cols),
        vert_loc,
        obs_source.reshape(1, obs),
        obs_column.reshape(1, obs),
        obs_slot.reshape(1, obs),
        obs_frac.reshape(1, obs),
        obs_count,
    )


def solution(mesh):
    placed = (
        P("member", None, None, "tile"),
        P("member", None, "tile"),
        P(),
        P("tile", None),
        P("tile"),
        P("tile"),
        P("tile"),
        P("tile"),
    )
    return jax.shard_map(
        on_device, mesh=mesh, in_specs=placed, out_specs=P(None, "tile"), check_vma=False
    )
```

```python
import functools

import jax
import jax.numpy as jnp
from jax import lax
from jax.experimental import pallas as pl
from jax.experimental.pallas import tpu as pltpu
from jax.sharding import PartitionSpec as P

MESH = pl.DeviceIdType.MESH
LANES = 128
F32 = jnp.float32
BF16 = jnp.bfloat16


def iota(shape, axis):
    return lax.broadcasted_iota(jnp.int32, shape, axis)


def one_hot(condition):
    return jnp.where(condition, F32(1.0), F32(0.0)).astype(BF16)


def dot(a, b):
    return jnp.dot(a, b, preferred_element_type=F32)


def dot_nt(a, b):
    return lax.dot_general(a, b, (((1,), (1,)), ((), ())), preferred_element_type=F32)


def two_pieces(x):
    high = x.astype(BF16)
    return high, (x - high.astype(F32)).astype(BF16)


def turned(x, shift):
    shift = shift % LANES
    return x if shift == 0 else pltpu.roll(x, shift, 1)


def kernel(
    tiles, groups, near, cap, packs,
    ens_hbm, ctl_hbm, vloc_hbm, source_hbm, column_hbm, slot_hbm, frac_hbm, count_ref,
    out_ref,
    vloc_ref, source_ref, column_ref, slot_ref, frac_ref, ens, ctl, weighted, part, part_in, asked, relay, req_in, res_out, res_in, place,
    load_sem, far_in, part_send, part_recv, near_send, near_recv, far_send, far_recv, res_send, res_recv,
):
    me = lax.axis_index("tile")
    mine = lax.axis_index("member")
    leader = groups - 1
    collector = leader - 1
    leads = mine == leader
    members, slots, levels, cols = ens.shape
    rows = levels // packs
    obs = column_ref.shape[1]
    owners = LANES // cap
    far = tiles // near
    low, high = lax.rem(me, near), me // near
    chunk = max(near, owners)
    chunks = tiles // chunk
    lines = chunk // near
    spans = chunk // owners
    width = spans * LANES

    def loaded(index, source, target):
        return pltpu.make_async_copy(source, target, load_sem.at[index])

    loads = [
        loaded(0, source_hbm, source_ref), loaded(1, column_hbm, column_ref),
        loaded(2, slot_hbm, slot_ref), loaded(3, frac_hbm, frac_ref),
        loaded(4, vloc_hbm, vloc_ref), loaded(5, ctl_hbm, ctl), loaded(6, ens_hbm, ens),
    ]

    def near_peer(step):
        return lax.rem(low + step, near)

    def far_peer(step):
        return lax.rem(high + step, far)

    barrier = pltpu.get_barrier_semaphore()

    def greet(tile, member):
        pl.semaphore_signal(
            barrier, inc=1, device_id={"tile": tile, "member": member}, device_id_type=MESH
        )

    @pl.when(leads)
    def _():
        for step in range(far - 1, 0, -1):
            greet(far_peer(step) * near + low, collector)
        for step in range(1, near):
            greet(high * near + near_peer(step), leader)
        for member in range(leader):
            greet(me, member)

    @pl.when(jnp.logical_not(leads))
    def _():
        greet(me, leader)

    for load in loads:
        load.start()

    def near_copy(peer, line):
        return pltpu.make_async_remote_copy(
            src_ref=asked.at[peer], dst_ref=relay.at[line],
            send_sem=near_send, recv_sem=near_recv.at[line],
            device_id={"tile": high * near + peer, "member": leader}, device_id_type=MESH,
        )

    def ranked():
        source = source_ref[...]
        hits = source == iota((tiles, obs), 0)
        hits_f = jnp.where(hits, F32(1.0), F32(0.0))
        before = one_hot(iota((LANES, LANES), 0) < iota((LANES, LANES), 1))
        seen = jnp.zeros((tiles, 1), F32)
        ranks = []
        for block in range(obs // LANES):
            hit = hits_f[:, block * LANES:(block + 1) * LANES]
            ahead = dot(hit.astype(BF16), before) + seen
            ranks.append(jnp.sum(ahead * hit, axis=0, keepdims=True))
            seen = seen + jnp.sum(hit, axis=1, keepdims=True)
        rank = jnp.concatenate(ranks, axis=1).astype(jnp.int32)
        return source, hits, rank

    for load in loads[:4]:
        load.wait()

    @pl.when(leads)
    def _():
        source, hits, rank = ranked()
        spread = one_hot(rank == lax.rem(iota((LANES, obs), 0), cap))
        frac = frac_ref[...]
        frac_0 = frac.astype(BF16).astype(F32)
        frac_1 = (frac - frac_0).astype(BF16).astype(F32)
        frac_2 = frac - frac_0 - frac_1
        values = [column_ref[...].astype(F32), slot_ref[...].astype(F32), frac_0, frac_1, frac_2]
        packed = dot_nt(
            jnp.concatenate([jnp.where(hits, v, F32(0.0)) for v in values], axis=0).astype(BF16), spread
        )
        packed = [packed[i * tiles:(i + 1) * tiles] for i in range(len(values))]
        seat = iota((tiles, LANES), 1) // cap == lax.rem(me, owners)
        code = jnp.where(seat, packed[0] + cols * packed[1], F32(0.0))
        part_of = jnp.where(seat, packed[2] + packed[3] + packed[4], F32(0.0))
        for tile in range(tiles):
            asked[tile % near, tile // near, 0:1] = code[tile:tile + 1]
            asked[tile % near, tile // near, 1:2] = part_of[tile:tile + 1]
        place[...] = one_hot(source * cap + rank == iota((tiles * cap, obs), 0))
        pl.semaphore_wait(barrier, near + groups - 2)
        for step in range(1, near):
            near_copy(near_peer(step), low).start()
        relay[low] = asked[low]

    batch = max(d for d in range(1, max(1, LANES // levels) + 1) if members % d == 0)
    wide = batch * levels
    repeat = one_hot(lax.rem(iota((wide, levels), 0), levels) == iota((wide, levels), 1))
    for load in loads[4:6]:
        load.wait()
    tall = dot(repeat, vloc_ref[...]).astype(BF16)
    full = dot_nt(tall, repeat)
    factor = jnp.where(
        iota((wide, wide), 0) // levels == iota((wide, wide), 1) // levels, full, F32(0.0)
    ).astype(BF16)
    for step in range(members // batch):
        weighted[step * wide:(step + 1) * wide] = dot(factor, ctl[step * wide:(step + 1) * wide])

    loads[6].wait()
    for slot in range(slots):
        total = jnp.zeros((levels, cols), F32)
        for k in range(members):
            total = total + ens[k, slot].astype(F32) * weighted[k * levels:(k + 1) * levels]
        part[slot * levels:(slot + 1) * levels] = total

    def give(member):
        return pltpu.make_async_remote_copy(
            src_ref=part, dst_ref=part_in.at[member],
            send_sem=part_send, recv_sem=part_recv.at[member],
            device_id={"tile": me, "member": leader}, device_id_type=MESH,
        )

    @pl.when(jnp.logical_not(leads))
    def _():
        gathers = mine == collector
        pl.semaphore_wait(barrier, jnp.where(gathers, far, 1))
        give(mine).start()

        @pl.when(gathers)
        def _():
            pl.semaphore_signal(
                far_in, inc=1, device_id={"tile": me, "member": leader}, device_id_type=MESH
            )

        source, _, rank = ranked()
        place[...] = one_hot(source * cap + rank == iota((tiles * cap, obs), 0))

    lane = iota((1, LANES), 1)
    stride = jnp.where(2 * me < tiles, 1, chunks - 1)
    home = me // chunk

    def chunk_at(step):
        return lax.rem(home + stride * step, chunks)

    def served(step):
        return home if step == 0 else jnp.where(step - 1 < home, step - 1, step)

    def unless(step, condition, body):
        if step == 0:
            pl.when(condition)(body)
        else:
            body()

    def reply_to(tile, member):
        return pltpu.make_async_remote_copy(
            src_ref=res_out.at[tile], dst_ref=res_in.at[me],
            send_sem=res_send.at[member], recv_sem=res_recv.at[home],
            device_id={"tile": tile, "member": member}, device_id_type=MESH,
        )

    def landed(source, target, send, recv):
        return pltpu.make_async_remote_copy(
            src_ref=source, dst_ref=target, send_sem=send, recv_sem=recv,
            device_id={"tile": me, "member": leader}, device_id_type=MESH,
        )

    @pl.when(leads)
    def _():
        def far_copy(peer, line):
            return pltpu.make_async_remote_copy(
                src_ref=relay.at[:, peer], dst_ref=req_in.at[pl.ds(line * near, near)],
                send_sem=far_send, recv_sem=far_recv.at[line],
                device_id={"tile": peer * near + low, "member": leader}, device_id_type=MESH,
            )

        for step in range(1, near):
            near_copy(near_peer(step), near_peer(step)).wait_recv()
        pl.semaphore_wait(far_in, 1)
        for step in range(1, far):
            far_copy(far_peer(step), high).start()
        req_in[pl.ds(high * near, near)] = relay[:, high]

        increment = part[...]
        for member in range(leader):
            give(member).wait_recv()
            increment = increment + part_in[member]
        pieces = jnp.concatenate(two_pieces(increment), axis=1)

        for step in range(chunks):
            group = served(step)
            for i in range(lines):
                line = group * lines + i
                unless(step, line != high, lambda line=line: far_copy(line, line).wait_recv())
            codes, fracs = [], []
            for s in range(spans):
                first = group * chunk + s * owners
                code, frac = req_in[first, 0:1], req_in[first, 1:2]
                for i in range(1, owners):
                    code = code + req_in[first + i, 0:1]
                    frac = frac + req_in[first + i, 1:2]
                codes.append(code)
                fracs.append(frac)
            code = jnp.concatenate(codes, axis=1).astype(jnp.int32)
            frac = jnp.concatenate(fracs, axis=1)
            wanted = code // cols
            column = code - wanted * cols
            pick = one_hot(iota((cols, width), 0) == column)
            columns = dot(pieces, jnp.concatenate([pick, pick], axis=0))
            answer = jnp.zeros((levels, width), F32)
            for slot in range(slots):
                weight = jnp.where(
                    wanted == slot, 1.0 - frac, jnp.where(wanted + 1 == slot, frac, F32(0.0))
                )
                answer = answer + weight * columns[slot * levels:(slot + 1) * levels]
            for t in range(chunk):
                s, i = t // owners, t % owners
                tile = group * chunk + t
                packet = jnp.zeros((rows, LANES), F32)
                for j in range(packs):
                    block = answer[j * rows:(j + 1) * rows, s * LANES:(s + 1) * LANES]
                    packet = jnp.where(lane // cap == j, turned(block, (j - i) * cap), packet)
                res_out[tile] = packet
                if step == 0:
                    @pl.when(tile == me)
                    def _():
                        res_in[me] = packet
                for member in range(leader):
                    reply_to(tile, member).start()
            for t in range(chunk):
                tile = group * chunk + t
                unless(step, tile != me, lambda tile=tile: reply_to(tile, leader).start())

    both = jnp.zeros((2 * levels, obs), F32)
    for step in range(chunks):
        group = chunk_at(step)
        whole = res_in.at[pl.ds(group * chunk, chunk)]
        if step == 0:
            if chunk > 1:
                @pl.when(leads)
                def _():
                    rest = res_in.at[pl.ds(0, chunk - 1)]
                    landed(rest, rest, res_send.at[leader], res_recv.at[group]).wait_recv()

            @pl.when(jnp.logical_not(leads))
            def _():
                landed(whole, whole, res_send.at[leader], res_recv.at[group]).wait_recv()
        else:
            landed(whole, whole, res_send.at[leader], res_recv.at[group]).wait_recv()
        columns = []
        for s in range(spans):
            bands = [jnp.zeros((rows, LANES), F32)] * packs
            for i in range(owners):
                got = res_in[group * chunk + s * owners + i]
                for j in range(packs):
                    bands[j] = jnp.where(lane // cap == i, turned(got, (i - j) * cap), bands[j])
            columns.append(jnp.concatenate(bands, axis=0))
        upper, lower = two_pieces(jnp.concatenate(columns, axis=1))
        first = pl.multiple_of(group * width, LANES)
        both = both + dot(jnp.concatenate([upper, lower], axis=0), place[pl.ds(first, width)])
    live = iota((levels, obs), 1) < count_ref[0]
    out_ref[...] = jnp.where(live, both[:levels] + both[levels:], F32(0.0))

    @pl.when(jnp.logical_not(leads))
    def _():
        give(mine).wait_send()

    @pl.when(leads)
    def _():
        def sent(buffer, sem):
            landed(buffer, buffer, sem, far_recv.at[0]).wait_send()

        if near > 1:
            sent(asked.at[pl.ds(0, near - 1)], near_send)
        if far > 1:
            sent(req_in.at[pl.ds(0, (far - 1) * near)], far_send)
        for member in range(leader):
            sent(res_out, res_send.at[member])
        if tiles > 1:
            sent(res_out.at[pl.ds(0, tiles - 1)], res_send.at[leader])


def on_device(ensemble, control, vert_loc, obs_source, obs_column, obs_slot, obs_frac, obs_count):
    tiles, groups = lax.axis_size("tile"), lax.axis_size("member")
    members, slots, levels, cols = ensemble.shape
    obs = obs_column.shape[0]
    cap = max(4, 2 * obs // tiles)
    near = max(d for d in range(1, tiles + 1) if tiles % d == 0 and d * d <= tiles)
    packs = max(1, min(LANES // cap, levels // 8))
    rows = levels // packs
    chunks = tiles // max(near, LANES // cap)
    vmem = pl.BlockSpec(memory_space=pltpu.VMEM)
    hbm = pl.BlockSpec(memory_space=pl.ANY)
    dma = pltpu.SemaphoreType.DMA
    return pl.pallas_call(
        functools.partial(kernel, tiles, groups, near, cap, packs),
        out_shape=pltpu.VMEM((levels, obs), F32),
        in_specs=[hbm] * 7 + [pl.BlockSpec(memory_space=pltpu.SMEM)],
        out_specs=vmem,
        scratch_shapes=[
            pltpu.VMEM((levels, levels), BF16),
            pltpu.VMEM((1, obs), jnp.int32),
            pltpu.VMEM((1, obs), jnp.int32),
            pltpu.VMEM((1, obs), jnp.int32),
            pltpu.VMEM((1, obs), F32),
            pltpu.VMEM((members, slots, levels, cols), BF16),
            pltpu.VMEM((members * levels, cols), BF16),
            pltpu.VMEM((members * levels, cols), F32),
            pltpu.VMEM((slots * levels, cols), F32),
            pltpu.VMEM((max(1, groups - 1), slots * levels, cols), F32),
            pltpu.VMEM((near, tiles // near, 2, LANES), F32),
            pltpu.VMEM((near, tiles // near, 2, LANES), F32),
            pltpu.VMEM((tiles, 2, LANES), F32),
            pltpu.VMEM((tiles, rows, LANES), F32),
            pltpu.VMEM((tiles, rows, LANES), F32),
            pltpu.VMEM((tiles * cap, obs), BF16),
            dma((7,)),
            pltpu.SemaphoreType.REGULAR,
            dma,
            dma((max(1, groups - 1),)),
            dma,
            dma((near,)),
            dma,
            dma((tiles // near,)),
            dma((groups,)),
            dma((chunks,)),
        ],
        compiler_params=pltpu.CompilerParams(collective_id=0, has_side_effects=True),
    )(
        ensemble,
        control.reshape(members * levels, cols),
        vert_loc,
        obs_source.reshape(1, obs),
        obs_column.reshape(1, obs),
        obs_slot.reshape(1, obs),
        obs_frac.reshape(1, obs),
        obs_count,
    )


def solution(mesh):
    placed = (
        P("member", None, None, "tile"),
        P("member", None, "tile"),
        P(),
        P("tile", None),
        P("tile"),
        P("tile"),
        P("tile"),
        P("tile"),
    )
    return jax.shard_map(
        on_device, mesh=mesh, in_specs=placed, out_specs=P(None, "tile"), check_vma=False
    )
```

```python
import functools

import jax
import jax.numpy as jnp
from jax import lax
from jax.experimental import pallas as pl
from jax.experimental.pallas import tpu as pltpu
from jax.sharding import PartitionSpec as P

MESH = pl.DeviceIdType.MESH
LANES = 128
F32 = jnp.float32
BF16 = jnp.bfloat16


def iota(shape, axis):
    return lax.broadcasted_iota(jnp.int32, shape, axis)


def one_hot(condition):
    return jnp.where(condition, F32(1.0), F32(0.0)).astype(BF16)


def dot(a, b):
    return jnp.dot(a, b, preferred_element_type=F32)


def dot_nt(a, b):
    return lax.dot_general(a, b, (((1,), (1,)), ((), ())), preferred_element_type=F32)


def two_pieces(x):
    high = x.astype(BF16)
    return high, (x - high.astype(F32)).astype(BF16)


def turned(x, shift):
    shift = shift % LANES
    return x if shift == 0 else pltpu.roll(x, shift, 1)


def kernel(
    tiles, groups, near, cap, packs,
    ens_hbm, ctl_hbm, vloc_hbm, source_hbm, column_hbm, slot_hbm, frac_hbm, count_ref,
    out_ref,
    vloc_ref, source_ref, column_ref, slot_ref, frac_ref, ens, ctl, weighted, part, part_in, asked, relay, req_in, res_out, res_in, place,
    rest_in, part_recv, near_recv, far_recv, res_recv,
    load_sem, part_send, near_send, far_send, res_send,
):
    me = lax.axis_index("tile")
    mine = lax.axis_index("member")
    leader = groups - 1
    collector = leader - 1
    leads = mine == leader
    members, slots, levels, cols = ens.shape
    rows = levels // packs
    obs = column_ref.shape[1]
    owners = LANES // cap
    far = tiles // near
    low, high = lax.rem(me, near), me // near
    chunk = max(near, owners)
    chunks = tiles // chunk
    lines = chunk // near
    spans = chunk // owners
    width = spans * LANES

    def loaded(index, source, target):
        return pltpu.make_async_copy(source, target, load_sem.at[index])

    loads = [
        loaded(0, source_hbm, source_ref), loaded(1, column_hbm, column_ref),
        loaded(2, slot_hbm, slot_ref), loaded(3, frac_hbm, frac_ref),
        loaded(4, vloc_hbm, vloc_ref), loaded(5, ctl_hbm, ctl), loaded(6, ens_hbm, ens),
    ]

    def near_peer(step):
        return lax.rem(low + step, near)

    def far_peer(step):
        return lax.rem(high + step, far)

    barrier = pltpu.get_barrier_semaphore()

    def greet(tile, member):
        pl.semaphore_signal(
            barrier, inc=1, device_id={"tile": tile, "member": member}, device_id_type=MESH
        )

    def taker(digit, direct):
        return jnp.where((digit == 0) == direct, leader, collector)

    @pl.when(leads)
    def _():
        for step in range(1, far):
            greet(far_peer(step) * near + low, taker(low, False))
        for step in range(near - 1, 0, -1):
            greet(high * near + near_peer(step), taker(near_peer(step), True))
        for member in range(leader):
            greet(me, member)

    @pl.when(jnp.logical_not(leads) & ((mine != collector) | (low == 0)))
    def _():
        greet(me, taker(low, True))

    for load in loads:
        load.start()

    def near_copy(peer, line):
        return pltpu.make_async_remote_copy(
            src_ref=asked.at[peer], dst_ref=relay.at[line],
            send_sem=near_send, recv_sem=near_recv.at[line],
            device_id={"tile": high * near + peer, "member": leader}, device_id_type=MESH,
        )

    def ranked():
        source = source_ref[...]
        hits = source == iota((tiles, obs), 0)
        hits_f = jnp.where(hits, F32(1.0), F32(0.0))
        before = one_hot(iota((LANES, LANES), 0) < iota((LANES, LANES), 1))
        seen = jnp.zeros((tiles, 1), F32)
        ranks = []
        for block in range(obs // LANES):
            hit = hits_f[:, block * LANES:(block + 1) * LANES]
            ahead = dot(hit.astype(BF16), before) + seen
            ranks.append(jnp.sum(ahead * hit, axis=0, keepdims=True))
            seen = seen + jnp.sum(hit, axis=1, keepdims=True)
        rank = jnp.concatenate(ranks, axis=1).astype(jnp.int32)
        return source, hits, rank

    for load in loads[:4]:
        load.wait()

    @pl.when(leads)
    def _():
        source, hits, rank = ranked()
        spread = one_hot(rank == lax.rem(iota((LANES, obs), 0), cap))
        frac = frac_ref[...]
        frac_0 = frac.astype(BF16).astype(F32)
        frac_1 = (frac - frac_0).astype(BF16).astype(F32)
        frac_2 = frac - frac_0 - frac_1
        values = [column_ref[...].astype(F32), slot_ref[...].astype(F32), frac_0, frac_1, frac_2]
        packed = dot_nt(
            jnp.concatenate([jnp.where(hits, v, F32(0.0)) for v in values], axis=0).astype(BF16), spread
        )
        packed = [packed[i * tiles:(i + 1) * tiles] for i in range(len(values))]
        seat = iota((tiles, LANES), 1) // cap == lax.rem(me, owners)
        code = jnp.where(seat, packed[0] + cols * packed[1], F32(0.0))
        part_of = jnp.where(seat, packed[2] + packed[3] + packed[4], F32(0.0))
        for tile in range(tiles):
            asked[tile % near, tile // near, 0:1] = code[tile:tile + 1]
            asked[tile % near, tile // near, 1:2] = part_of[tile:tile + 1]

        @pl.when(low == 0)
        def _():
            pl.semaphore_wait(barrier, near + groups - 2)

        @pl.when(low != 0)
        def _():
            pl.semaphore_wait(rest_in, 1)

        for step in range(1, near):
            near_copy(near_peer(step), low).start()
        relay[low] = asked[low]
        place[...] = one_hot(source * cap + rank == iota((tiles * cap, obs), 0))

    def entered(count):
        pl.semaphore_wait(barrier, count)
        pl.semaphore_signal(
            rest_in, inc=1, device_id={"tile": me, "member": leader}, device_id_type=MESH
        )

    @pl.when((mine == collector) & (low != 0))
    def _():
        entered(near + groups - 2)

    batch = max(d for d in range(1, max(1, LANES // levels) + 1) if members % d == 0)
    wide = batch * levels
    repeat = one_hot(lax.rem(iota((wide, levels), 0), levels) == iota((wide, levels), 1))
    for load in loads[4:6]:
        load.wait()
    tall = dot(repeat, vloc_ref[...]).astype(BF16)
    full = dot_nt(tall, repeat)
    factor = jnp.where(
        iota((wide, wide), 0) // levels == iota((wide, wide), 1) // levels, full, F32(0.0)
    ).astype(BF16)
    for step in range(members // batch):
        weighted[step * wide:(step + 1) * wide] = dot(factor, ctl[step * wide:(step + 1) * wide])

    loads[6].wait()
    for slot in range(slots):
        total = jnp.zeros((levels, cols), F32)
        for k in range(members):
            total = total + ens[k, slot].astype(F32) * weighted[k * levels:(k + 1) * levels]
        part[slot * levels:(slot + 1) * levels] = total

    def give(member):
        return pltpu.make_async_remote_copy(
            src_ref=part, dst_ref=part_in.at[member],
            send_sem=part_send, recv_sem=part_recv.at[member],
            device_id={"tile": me, "member": leader}, device_id_type=MESH,
        )

    @pl.when(jnp.logical_not(leads))
    def _():
        @pl.when((mine == collector) & (low == 0))
        def _():
            entered(far)

        @pl.when(mine != collector)
        def _():
            pl.semaphore_wait(barrier, 1)

        give(mine).start()
        source, _, rank = ranked()
        place[...] = one_hot(source * cap + rank == iota((tiles * cap, obs), 0))

    lane = iota((1, LANES), 1)
    stride = jnp.where(2 * me < tiles, 1, chunks - 1)
    home = me // chunk

    def chunk_at(step):
        return lax.rem(home + stride * step, chunks)

    def served(step):
        return home if step == 0 else jnp.where(step - 1 < home, step - 1, step)

    def unless(step, condition, body):
        if step == 0:
            pl.when(condition)(body)
        else:
            body()

    def reply_to(tile, member):
        return pltpu.make_async_remote_copy(
            src_ref=res_out.at[tile], dst_ref=res_in.at[me],
            send_sem=res_send.at[member], recv_sem=res_recv.at[home],
            device_id={"tile": tile, "member": member}, device_id_type=MESH,
        )

    def landed(source, target, send, recv):
        return pltpu.make_async_remote_copy(
            src_ref=source, dst_ref=target, send_sem=send, recv_sem=recv,
            device_id={"tile": me, "member": leader}, device_id_type=MESH,
        )

    @pl.when(leads)
    def _():
        def far_copy(peer, line):
            return pltpu.make_async_remote_copy(
                src_ref=relay.at[:, peer], dst_ref=req_in.at[pl.ds(line * near, near)],
                send_sem=far_send, recv_sem=far_recv.at[line],
                device_id={"tile": peer * near + low, "member": leader}, device_id_type=MESH,
            )

        for step in range(1, near):
            near_copy(near_peer(step), near_peer(step)).wait_recv()

        @pl.when(low == 0)
        def _():
            pl.semaphore_wait(rest_in, 1)

        @pl.when(low != 0)
        def _():
            pl.semaphore_wait(barrier, far - 1)

        for step in range(1, far):
            far_copy(far_peer(step), high).start()
        req_in[pl.ds(high * near, near)] = relay[:, high]

        increment = part[...]
        for member in range(leader):
            give(member).wait_recv()
            increment = increment + part_in[member]
        pieces = jnp.concatenate(two_pieces(increment), axis=1)

        for step in range(chunks):
            group = served(step)
            for i in range(lines):
                line = group * lines + i
                unless(step, line != high, lambda line=line: far_copy(line, line).wait_recv())
            codes, fracs = [], []
            for s in range(spans):
                first = group * chunk + s * owners
                code, frac = req_in[first, 0:1], req_in[first, 1:2]
                for i in range(1, owners):
                    code = code + req_in[first + i, 0:1]
                    frac = frac + req_in[first + i, 1:2]
                codes.append(code)
                fracs.append(frac)
            code = jnp.concatenate(codes, axis=1).astype(jnp.int32)
            frac = jnp.concatenate(fracs, axis=1)
            wanted = code // cols
            column = code - wanted * cols
            pick = one_hot(iota((cols, width), 0) == column)
            columns = dot(pieces, jnp.concatenate([pick, pick], axis=0))
            answer = jnp.zeros((levels, width), F32)
            for slot in range(slots):
                weight = jnp.where(
                    wanted == slot, 1.0 - frac, jnp.where(wanted + 1 == slot, frac, F32(0.0))
                )
                answer = answer + weight * columns[slot * levels:(slot + 1) * levels]
            for t in range(chunk):
                s, i = t // owners, t % owners
                tile = group * chunk + t
                packet = jnp.zeros((rows, LANES), F32)
                for j in range(packs):
                    block = answer[j * rows:(j + 1) * rows, s * LANES:(s + 1) * LANES]
                    packet = jnp.where(lane // cap == j, turned(block, (j - i) * cap), packet)
                res_out[tile] = packet
                if step == 0:
                    @pl.when(tile == me)
                    def _():
                        res_in[me] = packet
                for member in range(leader):
                    reply_to(tile, member).start()
            for t in range(chunk):
                tile = group * chunk + t
                unless(step, tile != me, lambda tile=tile: reply_to(tile, leader).start())

    both = jnp.zeros((2 * levels, obs), F32)
    for step in range(chunks):
        group = chunk_at(step)
        whole = res_in.at[pl.ds(group * chunk, chunk)]
        if step == 0:
            if chunk > 1:
                @pl.when(leads)
                def _():
                    rest = res_in.at[pl.ds(0, chunk - 1)]
                    landed(rest, rest, res_send.at[leader], res_recv.at[group]).wait_recv()

            @pl.when(jnp.logical_not(leads))
            def _():
                landed(whole, whole, res_send.at[leader], res_recv.at[group]).wait_recv()
        else:
            landed(whole, whole, res_send.at[leader], res_recv.at[group]).wait_recv()
        columns = []
        for s in range(spans):
            bands = [jnp.zeros((rows, LANES), F32)] * packs
            for i in range(owners):
                got = res_in[group * chunk + s * owners + i]
                for j in range(packs):
                    bands[j] = jnp.where(lane // cap == i, turned(got, (i - j) * cap), bands[j])
            columns.append(jnp.concatenate(bands, axis=0))
        upper, lower = two_pieces(jnp.concatenate(columns, axis=1))
        first = pl.multiple_of(group * width, LANES)
        both = both + dot(jnp.concatenate([upper, lower], axis=0), place[pl.ds(first, width)])
    live = iota((levels, obs), 1) < count_ref[0]
    out_ref[...] = jnp.where(live, both[:levels] + both[levels:], F32(0.0))

    @pl.when(jnp.logical_not(leads))
    def _():
        give(mine).wait_send()

    @pl.when(leads)
    def _():
        def sent(buffer, sem):
            landed(buffer, buffer, sem, far_recv.at[0]).wait_send()

        if near > 1:
            sent(asked.at[pl.ds(0, near - 1)], near_send)
        if far > 1:
            sent(req_in.at[pl.ds(0, (far - 1) * near)], far_send)
        for member in range(leader):
            sent(res_out, res_send.at[member])
        if tiles > 1:
            sent(res_out.at[pl.ds(0, tiles - 1)], res_send.at[leader])


def scoped(*args):
    dma = pltpu.SemaphoreType.DMA
    pl.run_scoped(
        functools.partial(kernel, *args), dma((7,)), dma(()), dma(()), dma(()), dma((args[1],))
    )


def on_device(ensemble, control, vert_loc, obs_source, obs_column, obs_slot, obs_frac, obs_count):
    tiles, groups = lax.axis_size("tile"), lax.axis_size("member")
    members, slots, levels, cols = ensemble.shape
    obs = obs_column.shape[0]
    cap = max(4, 2 * obs // tiles)
    near = max(d for d in range(1, tiles + 1) if tiles % d == 0 and d * d <= tiles)
    packs = max(1, min(LANES // cap, levels // 8))
    rows = levels // packs
    chunks = tiles // max(near, LANES // cap)
    vmem = pl.BlockSpec(memory_space=pltpu.VMEM)
    hbm = pl.BlockSpec(memory_space=pl.ANY)
    dma = pltpu.SemaphoreType.DMA
    return pl.pallas_call(
        functools.partial(scoped, tiles, groups, near, cap, packs),
        out_shape=pltpu.VMEM((levels, obs), F32),
        in_specs=[hbm] * 7 + [pl.BlockSpec(memory_space=pltpu.SMEM)],
        out_specs=vmem,
        scratch_shapes=[
            pltpu.VMEM((levels, levels), BF16),
            pltpu.VMEM((1, obs), jnp.int32),
            pltpu.VMEM((1, obs), jnp.int32),
            pltpu.VMEM((1, obs), jnp.int32),
            pltpu.VMEM((1, obs), F32),
            pltpu.VMEM((members, slots, levels, cols), BF16),
            pltpu.VMEM((members * levels, cols), BF16),
            pltpu.VMEM((members * levels, cols), F32),
            pltpu.VMEM((slots * levels, cols), F32),
            pltpu.VMEM((max(1, groups - 1), slots * levels, cols), F32),
            pltpu.VMEM((near, tiles // near, 2, LANES), F32),
            pltpu.VMEM((near, tiles // near, 2, LANES), F32),
            pltpu.VMEM((tiles, 2, LANES), F32),
            pltpu.VMEM((tiles, rows, LANES), F32),
            pltpu.VMEM((tiles, rows, LANES), F32),
            pltpu.VMEM((tiles * cap, obs), BF16),
            pltpu.SemaphoreType.REGULAR,
            dma((max(1, groups - 1),)),
            dma((near,)),
            dma((tiles // near,)),
            dma((chunks,)),
        ],
        compiler_params=pltpu.CompilerParams(collective_id=0, has_side_effects=True),
    )(
        ensemble,
        control.reshape(members * levels, cols),
        vert_loc,
        obs_source.reshape(1, obs),
        obs_column.reshape(1, obs),
        obs_slot.reshape(1, obs),
        obs_frac.reshape(1, obs),
        obs_count,
    )


def solution(mesh):
    placed = (
        P("member", None, None, "tile"),
        P("member", None, "tile"),
        P(),
        P("tile", None),
        P("tile"),
        P("tile"),
        P("tile"),
        P("tile"),
    )
    return jax.shard_map(
        on_device, mesh=mesh, in_specs=placed, out_specs=P(None, "tile"), check_vma=False
    )
```

```python
import functools

import jax
import jax.numpy as jnp
from jax import lax
from jax.experimental import pallas as pl
from jax.experimental.pallas import tpu as pltpu
from jax.sharding import PartitionSpec as P

MESH = pl.DeviceIdType.MESH
LANES = 128
F32 = jnp.float32
BF16 = jnp.bfloat16


def iota(shape, axis):
    return lax.broadcasted_iota(jnp.int32, shape, axis)


def one_hot(condition):
    return jnp.where(condition, F32(1.0), F32(0.0)).astype(BF16)


def dot(a, b):
    return jnp.dot(a, b, preferred_element_type=F32)


def dot_nt(a, b):
    return lax.dot_general(a, b, (((1,), (1,)), ((), ())), preferred_element_type=F32)


def two_pieces(x):
    high = x.astype(BF16)
    return high, (x - high.astype(F32)).astype(BF16)


def turned(x, shift):
    shift = shift % LANES
    return x if shift == 0 else pltpu.roll(x, shift, 1)


def kernel(
    tiles, groups, near, cap, packs,
    ens_hbm, ctl_hbm, vloc_hbm, source_hbm, column_hbm, slot_hbm, frac_hbm, count_ref,
    out_ref,
    vloc_ref, source_ref, column_ref, slot_ref, frac_ref, ens, ctl, weighted, part, part_in, asked, relay, req_in, res_out, res_in, place,
    rest_in, part_recv, near_recv, far_recv, res_recv,
    load_sem, part_send, near_send, far_send, res_send,
):
    me = lax.axis_index("tile")
    mine = lax.axis_index("member")
    leader = groups - 1
    collector = leader - 1
    leads = mine == leader
    members, slots, levels, cols = ens.shape
    rows = levels // packs
    obs = column_ref.shape[1]
    owners = LANES // cap
    far = tiles // near
    low, high = lax.rem(me, near), me // near
    chunk = max(near, owners)
    chunks = tiles // chunk
    lines = chunk // near
    spans = chunk // owners
    width = spans * LANES

    def loaded(index, source, target):
        return pltpu.make_async_copy(source, target, load_sem.at[index])

    loads = [
        loaded(0, source_hbm, source_ref), loaded(1, column_hbm, column_ref),
        loaded(2, slot_hbm, slot_ref), loaded(3, frac_hbm, frac_ref),
        loaded(4, vloc_hbm, vloc_ref), loaded(5, ctl_hbm, ctl), loaded(6, ens_hbm, ens),
    ]

    def near_peer(step):
        return lax.rem(low + step, near)

    def far_peer(step):
        return lax.rem(high + step, far)

    barrier = pltpu.get_barrier_semaphore()

    def greet(tile, member):
        pl.semaphore_signal(
            barrier, inc=1, device_id={"tile": tile, "member": member}, device_id_type=MESH
        )

    def taker(digit, direct):
        return jnp.where((digit == 0) == direct, leader, collector)

    @pl.when(leads)
    def _():
        for step in range(1, near):
            greet(high * near + near_peer(step), taker(near_peer(step), True))
        for step in range(1, far):
            greet(far_peer(step) * near + low, taker(low, False))
        for member in range(leader):
            greet(me, member)

    @pl.when(jnp.logical_not(leads) & ((mine != collector) | (low == 0)))
    def _():
        greet(me, taker(low, True))

    for load in loads:
        load.start()

    def near_copy(peer, line):
        return pltpu.make_async_remote_copy(
            src_ref=asked.at[peer], dst_ref=relay.at[line],
            send_sem=near_send, recv_sem=near_recv,
            device_id={"tile": high * near + peer, "member": leader}, device_id_type=MESH,
        )

    def ranked():
        source = source_ref[...]
        hits = source == iota((tiles, obs), 0)
        hits_f = jnp.where(hits, F32(1.0), F32(0.0))
        before = one_hot(iota((LANES, LANES), 0) < iota((LANES, LANES), 1))
        seen = jnp.zeros((tiles, 1), F32)
        ranks = []
        for block in range(obs // LANES):
            hit = hits_f[:, block * LANES:(block + 1) * LANES]
            ahead = dot(hit.astype(BF16), before) + seen
            ranks.append(jnp.sum(ahead * hit, axis=0, keepdims=True))
            seen = seen + jnp.sum(hit, axis=1, keepdims=True)
        rank = jnp.concatenate(ranks, axis=1).astype(jnp.int32)
        return source, hits, rank

    def placed(source, rank):
        live = iota((1, obs), 1) < count_ref[0]
        position = jnp.where(live, source * cap + rank, -1)
        return one_hot(position == iota((tiles * cap, obs), 0))

    for load in loads[:4]:
        load.wait()

    @pl.when(leads)
    def _():
        source, hits, rank = ranked()
        spread = one_hot(rank == lax.rem(iota((LANES, obs), 0), cap))
        frac = frac_ref[...]
        frac_0 = frac.astype(BF16).astype(F32)
        frac_1 = (frac - frac_0).astype(BF16).astype(F32)
        frac_2 = frac - frac_0 - frac_1
        values = [column_ref[...].astype(F32), slot_ref[...].astype(F32), frac_0, frac_1, frac_2]
        packed = dot_nt(
            jnp.concatenate([jnp.where(hits, v, F32(0.0)) for v in values], axis=0).astype(BF16), spread
        )
        packed = [packed[i * tiles:(i + 1) * tiles] for i in range(len(values))]
        seat = iota((tiles, LANES), 1) // cap == lax.rem(me, owners)
        code = jnp.where(seat, packed[0] + cols * packed[1], F32(0.0))
        part_of = jnp.where(seat, packed[2] + packed[3] + packed[4], F32(0.0))
        for tile in range(tiles):
            asked[tile % near, tile // near, 0:1] = code[tile:tile + 1]
            asked[tile % near, tile // near, 1:2] = part_of[tile:tile + 1]

        @pl.when(low == 0)
        def _():
            pl.semaphore_wait(barrier, near + groups - 2)

        @pl.when(low != 0)
        def _():
            pl.semaphore_wait(rest_in, 1)

        for step in range(1, near):
            near_copy(near_peer(step), low).start()
        relay[low] = asked[low]
        place[...] = placed(source, rank)

    def entered(count):
        pl.semaphore_wait(barrier, count)
        pl.semaphore_signal(
            rest_in, inc=1, device_id={"tile": me, "member": leader}, device_id_type=MESH
        )

    @pl.when((mine == collector) & (low != 0))
    def _():
        entered(near + groups - 2)

    batch = max(d for d in range(1, max(1, LANES // levels) + 1) if members % d == 0)
    wide = batch * levels
    repeat = one_hot(lax.rem(iota((wide, levels), 0), levels) == iota((wide, levels), 1))
    for load in loads[4:6]:
        load.wait()
    tall = dot(repeat, vloc_ref[...]).astype(BF16)
    full = dot_nt(tall, repeat)
    factor = jnp.where(
        iota((wide, wide), 0) // levels == iota((wide, wide), 1) // levels, full, F32(0.0)
    ).astype(BF16)
    for step in range(members // batch):
        weighted[step * wide:(step + 1) * wide] = dot(factor, ctl[step * wide:(step + 1) * wide])

    loads[6].wait()
    for slot in range(slots):
        total = jnp.zeros((levels, cols), F32)
        for k in range(members):
            total = total + ens[k, slot].astype(F32) * weighted[k * levels:(k + 1) * levels]
        part[slot * levels:(slot + 1) * levels] = total

    def give(member):
        return pltpu.make_async_remote_copy(
            src_ref=part, dst_ref=part_in.at[member],
            send_sem=part_send, recv_sem=part_recv.at[member],
            device_id={"tile": me, "member": leader}, device_id_type=MESH,
        )

    @pl.when(jnp.logical_not(leads))
    def _():
        @pl.when((mine == collector) & (low == 0))
        def _():
            entered(far)

        @pl.when(mine != collector)
        def _():
            pl.semaphore_wait(barrier, 1)

        give(mine).start()
        source, _, rank = ranked()
        place[...] = placed(source, rank)

    lane = iota((1, LANES), 1)
    stride = jnp.where(2 * me < tiles, 1, chunks - 1)
    home = me // chunk

    def chunk_at(step):
        return lax.rem(home + stride * step, chunks)

    def served(step):
        return home if step == 0 else jnp.where(step - 1 < home, step - 1, step)

    def unless(step, condition, body):
        if step == 0:
            pl.when(condition)(body)
        else:
            body()

    def reply_to(tile, member):
        return pltpu.make_async_remote_copy(
            src_ref=res_out.at[tile], dst_ref=res_in.at[me],
            send_sem=res_send.at[member], recv_sem=res_recv.at[home],
            device_id={"tile": tile, "member": member}, device_id_type=MESH,
        )

    def landed(source, target, send, recv):
        return pltpu.make_async_remote_copy(
            src_ref=source, dst_ref=target, send_sem=send, recv_sem=recv,
            device_id={"tile": me, "member": leader}, device_id_type=MESH,
        )

    @pl.when(leads)
    def _():
        def far_copy(peer, line):
            return pltpu.make_async_remote_copy(
                src_ref=relay.at[:, peer], dst_ref=req_in.at[pl.ds(line * near, near)],
                send_sem=far_send, recv_sem=far_recv.at[line],
                device_id={"tile": peer * near + low, "member": leader}, device_id_type=MESH,
            )

        if near > 1:
            others = relay.at[pl.ds(0, near - 1)]
            landed(others, others, near_send, near_recv).wait_recv()

        @pl.when(low == 0)
        def _():
            pl.semaphore_wait(rest_in, 1)

        @pl.when(low != 0)
        def _():
            pl.semaphore_wait(barrier, far - 1)

        for step in range(1, far):
            far_copy(far_peer(step), high).start()
        req_in[pl.ds(high * near, near)] = relay[:, high]

        increment = part[...]
        for member in range(leader):
            give(member).wait_recv()
            increment = increment + part_in[member]
        pieces = jnp.concatenate(two_pieces(increment), axis=1)

        for step in range(chunks):
            group = served(step)
            for i in range(lines):
                line = group * lines + i
                unless(step, line != high, lambda line=line: far_copy(line, line).wait_recv())
            codes, fracs = [], []
            for s in range(spans):
                first = group * chunk + s * owners
                code, frac = req_in[first, 0:1], req_in[first, 1:2]
                for i in range(1, owners):
                    code = code + req_in[first + i, 0:1]
                    frac = frac + req_in[first + i, 1:2]
                codes.append(code)
                fracs.append(frac)
            code = jnp.concatenate(codes, axis=1).astype(jnp.int32)
            frac = jnp.concatenate(fracs, axis=1)
            wanted = code // cols
            column = code - wanted * cols
            pick = one_hot(iota((cols, width), 0) == column)
            columns = dot(pieces, jnp.concatenate([pick, pick], axis=0))
            answer = jnp.zeros((levels, width), F32)
            for slot in range(slots):
                weight = jnp.where(
                    wanted == slot, 1.0 - frac, jnp.where(wanted + 1 == slot, frac, F32(0.0))
                )
                answer = answer + weight * columns[slot * levels:(slot + 1) * levels]
            for t in range(chunk):
                s, i = t // owners, t % owners
                tile = group * chunk + t
                packet = jnp.zeros((rows, LANES), F32)
                for j in range(packs):
                    block = answer[j * rows:(j + 1) * rows, s * LANES:(s + 1) * LANES]
                    packet = jnp.where(lane // cap == j, turned(block, (j - i) * cap), packet)
                res_out[tile] = packet
                if step == 0:
                    @pl.when(tile == me)
                    def _():
                        res_in[me] = packet
                for member in range(leader):
                    reply_to(tile, member).start()
            for t in range(chunk):
                tile = group * chunk + t
                unless(step, tile != me, lambda tile=tile: reply_to(tile, leader).start())

    both = jnp.zeros((2 * levels, obs), F32)
    for step in range(chunks):
        group = chunk_at(step)
        whole = res_in.at[pl.ds(group * chunk, chunk)]
        if step == 0:
            if chunk > 1:
                @pl.when(leads)
                def _():
                    rest = res_in.at[pl.ds(0, chunk - 1)]
                    landed(rest, rest, res_send.at[leader], res_recv.at[group]).wait_recv()

            @pl.when(jnp.logical_not(leads))
            def _():
                landed(whole, whole, res_send.at[leader], res_recv.at[group]).wait_recv()
        else:
            landed(whole, whole, res_send.at[leader], res_recv.at[group]).wait_recv()
        columns = []
        for s in range(spans):
            bands = [jnp.zeros((rows, LANES), F32)] * packs
            for i in range(owners):
                got = res_in[group * chunk + s * owners + i]
                for j in range(packs):
                    bands[j] = jnp.where(lane // cap == i, turned(got, (i - j) * cap), bands[j])
            columns.append(jnp.concatenate(bands, axis=0))
        upper, lower = two_pieces(jnp.concatenate(columns, axis=1))
        first = pl.multiple_of(group * width, LANES)
        both = both + dot(jnp.concatenate([upper, lower], axis=0), place[pl.ds(first, width)])
    out_ref[...] = both[:levels] + both[levels:]

    @pl.when(jnp.logical_not(leads))
    def _():
        give(mine).wait_send()

    @pl.when(leads)
    def _():
        def sent(buffer, sem):
            landed(buffer, buffer, sem, far_recv.at[0]).wait_send()

        if near > 1:
            sent(asked.at[pl.ds(0, near - 1)], near_send)
        if far > 1:
            sent(req_in.at[pl.ds(0, (far - 1) * near)], far_send)
        for member in range(leader):
            sent(res_out, res_send.at[member])
        if tiles > 1:
            sent(res_out.at[pl.ds(0, tiles - 1)], res_send.at[leader])


def scoped(tiles, groups, near, cap, packs, *refs):
    dma = pltpu.SemaphoreType.DMA
    one, chunks = dma(()), tiles // max(near, LANES // cap)
    pl.run_scoped(
        functools.partial(kernel, tiles, groups, near, cap, packs, *refs),
        pltpu.SemaphoreType.REGULAR(()), dma((max(1, groups - 1),)), one, dma((tiles // near,)), dma((chunks,)),
        dma((7,)), one, one, one, dma((groups,)),
    )


def on_device(ensemble, control, vert_loc, obs_source, obs_column, obs_slot, obs_frac, obs_count):
    tiles, groups = lax.axis_size("tile"), lax.axis_size("member")
    members, slots, levels, cols = ensemble.shape
    obs = obs_column.shape[0]
    cap = max(4, 2 * obs // tiles)
    near = max(d for d in range(1, tiles + 1) if tiles % d == 0 and d * d <= tiles)
    packs = max(1, min(LANES // cap, levels // 8))
    rows = levels // packs
    vmem = pl.BlockSpec(memory_space=pltpu.VMEM)
    hbm = pl.BlockSpec(memory_space=pl.ANY)
    return pl.pallas_call(
        functools.partial(scoped, tiles, groups, near, cap, packs),
        out_shape=pltpu.VMEM((levels, obs), F32),
        in_specs=[hbm] * 7 + [pl.BlockSpec(memory_space=pltpu.SMEM)],
        out_specs=vmem,
        scratch_shapes=[
            pltpu.VMEM((levels, levels), BF16),
            pltpu.VMEM((1, obs), jnp.int32),
            pltpu.VMEM((1, obs), jnp.int32),
            pltpu.VMEM((1, obs), jnp.int32),
            pltpu.VMEM((1, obs), F32),
            pltpu.VMEM((members, slots, levels, cols), BF16),
            pltpu.VMEM((members * levels, cols), BF16),
            pltpu.VMEM((members * levels, cols), F32),
            pltpu.VMEM((slots * levels, cols), F32),
            pltpu.VMEM((max(1, groups - 1), slots * levels, cols), F32),
            pltpu.VMEM((near, tiles // near, 2, LANES), F32),
            pltpu.VMEM((near, tiles // near, 2, LANES), F32),
            pltpu.VMEM((tiles, 2, LANES), F32),
            pltpu.VMEM((tiles, rows, LANES), F32),
            pltpu.VMEM((tiles, rows, LANES), F32),
            pltpu.VMEM((tiles * cap, obs), BF16),
        ],
        compiler_params=pltpu.CompilerParams(collective_id=0, has_side_effects=True),
    )(
        ensemble,
        control.reshape(members * levels, cols),
        vert_loc,
        obs_source.reshape(1, obs),
        obs_column.reshape(1, obs),
        obs_slot.reshape(1, obs),
        obs_frac.reshape(1, obs),
        obs_count,
    )


def solution(mesh):
    placed = (
        P("member", None, None, "tile"),
        P("member", None, "tile"),
        P(),
        P("tile", None),
        P("tile"),
        P("tile"),
        P("tile"),
        P("tile"),
    )
    return jax.shard_map(
        on_device, mesh=mesh, in_specs=placed, out_specs=P(None, "tile"), check_vma=False
    )
```

```python
import functools

import jax
import jax.numpy as jnp
from jax import lax
from jax.experimental import pallas as pl
from jax.experimental.pallas import tpu as pltpu
from jax.sharding import PartitionSpec as P

MESH = pl.DeviceIdType.MESH
LANES = 128
F32 = jnp.float32
BF16 = jnp.bfloat16


def iota(shape, axis):
    return lax.broadcasted_iota(jnp.int32, shape, axis)


def one_hot(condition):
    return jnp.where(condition, F32(1.0), F32(0.0)).astype(BF16)


def dot(a, b):
    return jnp.dot(a, b, preferred_element_type=F32)


def dot_nt(a, b):
    return lax.dot_general(a, b, (((1,), (1,)), ((), ())), preferred_element_type=F32)


def two_pieces(x):
    high = x.astype(BF16)
    return high, (x - high.astype(F32)).astype(BF16)


def turned(x, shift):
    shift = shift % LANES
    return x if shift == 0 else pltpu.roll(x, shift, 1)


def kernel(
    tiles, groups, near, cap, packs,
    ens_hbm, ctl_hbm, vloc_hbm, source_hbm, column_hbm, slot_hbm, frac_hbm, count_ref,
    out_ref,
    vloc_ref, source_ref, column_ref, slot_ref, frac_ref, ens, ctl, weighted, part, part_in, asked, relay, req_in, res_out, res_in, place,
    rest_in, part_recv, near_recv, far_recv, res_recv,
    load_sem, part_send, near_send, far_send, res_send,
):
    me = lax.axis_index("tile")
    mine = lax.axis_index("member")
    leader = groups - 1
    collector = leader - 1
    leads = mine == leader
    members, slots, levels, cols = ens.shape
    rows = levels // packs
    obs = column_ref.shape[1]
    owners = LANES // cap
    far = tiles // near
    low, high = lax.rem(me, near), me // near
    chunk = max(near, owners)
    chunks = tiles // chunk
    lines = chunk // near
    spans = chunk // owners
    width = spans * LANES

    def loaded(index, source, target):
        return pltpu.make_async_copy(source, target, load_sem.at[index])

    loads = [
        loaded(0, source_hbm, source_ref), loaded(1, column_hbm, column_ref),
        loaded(2, slot_hbm, slot_ref), loaded(3, frac_hbm, frac_ref),
        loaded(4, vloc_hbm, vloc_ref), loaded(5, ctl_hbm, ctl), loaded(6, ens_hbm, ens),
    ]

    def near_peer(step):
        return lax.rem(low + step, near)

    def far_peer(step):
        return lax.rem(high + step, far)

    barrier = pltpu.get_barrier_semaphore()

    def greet(tile, member):
        pl.semaphore_signal(
            barrier, inc=1, device_id={"tile": tile, "member": member}, device_id_type=MESH
        )

    def taker(digit, direct):
        return jnp.where((digit == 0) == direct, leader, collector)

    @pl.when(leads)
    def _():
        for step in range(1, near):
            greet(high * near + near_peer(step), taker(near_peer(step), True))
        for step in range(1, far):
            greet(far_peer(step) * near + low, taker(low, False))
        for member in range(leader):
            greet(me, member)

    @pl.when(jnp.logical_not(leads) & ((mine != collector) | (low == 0)))
    def _():
        greet(me, taker(low, True))

    for load in loads:
        load.start()

    def near_copy(peer, line):
        return pltpu.make_async_remote_copy(
            src_ref=asked.at[peer], dst_ref=relay.at[line],
            send_sem=near_send, recv_sem=near_recv,
            device_id={"tile": high * near + peer, "member": leader}, device_id_type=MESH,
        )

    def ranked():
        source = source_ref[...]
        hits = source == iota((tiles, obs), 0)
        hits_f = jnp.where(hits, F32(1.0), F32(0.0))
        before = one_hot(iota((LANES, LANES), 0) < iota((LANES, LANES), 1))
        seen = jnp.zeros((tiles, 1), F32)
        ranks = []
        for block in range(obs // LANES):
            hit = hits_f[:, block * LANES:(block + 1) * LANES]
            ahead = dot(hit.astype(BF16), before) + seen
            ranks.append(jnp.sum(ahead * hit, axis=0, keepdims=True))
            seen = seen + jnp.sum(hit, axis=1, keepdims=True)
        rank = jnp.concatenate(ranks, axis=1).astype(jnp.int32)
        return source, hits, rank

    def placed(source, rank):
        live = iota((1, obs), 1) < count_ref[0]
        position = jnp.where(live, source * cap + rank, -1)
        return one_hot(position == iota((tiles * cap, obs), 0))

    for load in loads[:4]:
        load.wait()

    @pl.when(leads)
    def _():
        source, hits, rank = ranked()
        spread = one_hot(rank == lax.rem(iota((LANES, obs), 0), cap))
        frac = frac_ref[...]
        frac_0 = frac.astype(BF16).astype(F32)
        frac_1 = (frac - frac_0).astype(BF16).astype(F32)
        frac_2 = frac - frac_0 - frac_1
        values = [column_ref[...].astype(F32), slot_ref[...].astype(F32), frac_0, frac_1, frac_2]
        packed = dot_nt(
            jnp.concatenate([jnp.where(hits, v, F32(0.0)) for v in values], axis=0).astype(BF16), spread
        )
        packed = [packed[i * tiles:(i + 1) * tiles] for i in range(len(values))]
        seat = iota((tiles, LANES), 1) // cap == lax.rem(me, owners)
        code = jnp.where(seat, packed[0] + cols * packed[1], F32(0.0))
        part_of = jnp.where(seat, packed[2] + packed[3] + packed[4], F32(0.0))
        for tile in range(tiles):
            asked[tile % near, tile // near, 0:1] = code[tile:tile + 1]
            asked[tile % near, tile // near, 1:2] = part_of[tile:tile + 1]

        @pl.when(low == 0)
        def _():
            pl.semaphore_wait(barrier, near + groups - 2)

        @pl.when(low != 0)
        def _():
            pl.semaphore_wait(rest_in, 1)

        for step in range(near - 1, 0, -1):
            near_copy(near_peer(step), low).start()
        relay[low] = asked[low]
        place[...] = placed(source, rank)

    def entered(count):
        pl.semaphore_wait(barrier, count)
        pl.semaphore_signal(
            rest_in, inc=1, device_id={"tile": me, "member": leader}, device_id_type=MESH
        )

    @pl.when((mine == collector) & (low != 0))
    def _():
        entered(near + groups - 2)

    batch = max(d for d in range(1, max(1, LANES // levels) + 1) if members % d == 0)
    wide = batch * levels
    repeat = one_hot(lax.rem(iota((wide, levels), 0), levels) == iota((wide, levels), 1))
    for load in loads[4:6]:
        load.wait()
    tall = dot(repeat, vloc_ref[...]).astype(BF16)
    full = dot_nt(tall, repeat)
    factor = jnp.where(
        iota((wide, wide), 0) // levels == iota((wide, wide), 1) // levels, full, F32(0.0)
    ).astype(BF16)
    for step in range(members // batch):
        weighted[step * wide:(step + 1) * wide] = dot(factor, ctl[step * wide:(step + 1) * wide])

    loads[6].wait()
    for slot in range(slots):
        total = jnp.zeros((levels, cols), F32)
        for k in range(members):
            total = total + ens[k, slot].astype(F32) * weighted[k * levels:(k + 1) * levels]
        part[slot * levels:(slot + 1) * levels] = total

    def give(member):
        return pltpu.make_async_remote_copy(
            src_ref=part, dst_ref=part_in.at[member],
            send_sem=part_send, recv_sem=part_recv.at[member],
            device_id={"tile": me, "member": leader}, device_id_type=MESH,
        )

    @pl.when(jnp.logical_not(leads))
    def _():
        @pl.when((mine == collector) & (low == 0))
        def _():
            entered(far)

        @pl.when(mine != collector)
        def _():
            pl.semaphore_wait(barrier, 1)

        give(mine).start()
        source, _, rank = ranked()
        place[...] = placed(source, rank)

    lane = iota((1, LANES), 1)
    stride = jnp.where(2 * me < tiles, 1, chunks - 1)
    home = me // chunk

    def chunk_at(step):
        return lax.rem(home + stride * step, chunks)

    def served(step):
        return home if step == 0 else jnp.where(step - 1 < home, step - 1, step)

    def unless(step, condition, body):
        if step == 0:
            pl.when(condition)(body)
        else:
            body()

    def reply_to(tile, member):
        return pltpu.make_async_remote_copy(
            src_ref=res_out.at[tile], dst_ref=res_in.at[me],
            send_sem=res_send.at[member], recv_sem=res_recv.at[home],
            device_id={"tile": tile, "member": member}, device_id_type=MESH,
        )

    def landed(source, target, send, recv):
        return pltpu.make_async_remote_copy(
            src_ref=source, dst_ref=target, send_sem=send, recv_sem=recv,
            device_id={"tile": me, "member": leader}, device_id_type=MESH,
        )

    @pl.when(leads)
    def _():
        def far_copy(peer, line):
            return pltpu.make_async_remote_copy(
                src_ref=relay.at[:, peer], dst_ref=req_in.at[pl.ds(line * near, near)],
                send_sem=far_send, recv_sem=far_recv.at[line],
                device_id={"tile": peer * near + low, "member": leader}, device_id_type=MESH,
            )

        if near > 1:
            others = relay.at[pl.ds(0, near - 1)]
            landed(others, others, near_send, near_recv).wait_recv()

        @pl.when(low == 0)
        def _():
            pl.semaphore_wait(rest_in, 1)

        @pl.when(low != 0)
        def _():
            pl.semaphore_wait(barrier, far - 1)

        for step in range(far - 1, 0, -1):
            far_copy(far_peer(step), high).start()
        req_in[pl.ds(high * near, near)] = relay[:, high]

        increment = part[...]
        for member in range(leader):
            give(member).wait_recv()
            increment = increment + part_in[member]
        pieces = jnp.concatenate(two_pieces(increment), axis=1)

        for step in range(chunks):
            group = served(step)
            for i in range(lines):
                line = group * lines + i
                unless(step, line != high, lambda line=line: far_copy(line, line).wait_recv())
            answers = []
            for s in range(spans):
                first = group * chunk + s * owners
                code, frac = req_in[first, 0:1], req_in[first, 1:2]
                for i in range(1, owners):
                    code = code + req_in[first + i, 0:1]
                    frac = frac + req_in[first + i, 1:2]
                wanted = jnp.floor((code + 0.5) * (1.0 / cols))
                column = (code - cols * wanted).astype(jnp.int32)
                pick = one_hot(iota((cols, LANES), 0) == column)
                columns = dot(pieces, jnp.concatenate([pick, pick], axis=0))
                answer = jnp.zeros((levels, LANES), F32)
                for slot in range(slots):
                    weight = jnp.where(
                        wanted == slot, 1.0 - frac, jnp.where(wanted == slot - 1, frac, F32(0.0))
                    )
                    answer = answer + weight * columns[slot * levels:(slot + 1) * levels]
                answers.append(answer)
            for t in range(chunk):
                s, i = t // owners, t % owners
                tile = group * chunk + t
                packet = jnp.zeros((rows, LANES), F32)
                for j in range(packs):
                    block = answers[s][j * rows:(j + 1) * rows]
                    packet = jnp.where(lane // cap == j, turned(block, (j - i) * cap), packet)
                res_out[tile] = packet
                if step == 0:
                    @pl.when(tile == me)
                    def _():
                        res_in[me] = packet
                for member in range(leader):
                    reply_to(tile, member).start()
            for t in range(chunk):
                tile = group * chunk + t
                unless(step, tile != me, lambda tile=tile: reply_to(tile, leader).start())

    both = jnp.zeros((2 * levels, obs), F32)
    for step in range(chunks):
        group = chunk_at(step)
        whole = res_in.at[pl.ds(group * chunk, chunk)]
        if step == 0:
            if chunk > 1:
                @pl.when(leads)
                def _():
                    rest = res_in.at[pl.ds(0, chunk - 1)]
                    landed(rest, rest, res_send.at[leader], res_recv.at[group]).wait_recv()

            @pl.when(jnp.logical_not(leads))
            def _():
                landed(whole, whole, res_send.at[leader], res_recv.at[group]).wait_recv()
        else:
            landed(whole, whole, res_send.at[leader], res_recv.at[group]).wait_recv()
        columns = []
        for s in range(spans):
            bands = [jnp.zeros((rows, LANES), F32)] * packs
            for i in range(owners):
                got = res_in[group * chunk + s * owners + i]
                for j in range(packs):
                    bands[j] = jnp.where(lane // cap == i, turned(got, (i - j) * cap), bands[j])
            columns.append(jnp.concatenate(bands, axis=0))
        upper, lower = two_pieces(jnp.concatenate(columns, axis=1))
        first = pl.multiple_of(group * width, LANES)
        both = both + dot(jnp.concatenate([upper, lower], axis=0), place[pl.ds(first, width)])
    out_ref[...] = both[:levels] + both[levels:]

    @pl.when(jnp.logical_not(leads))
    def _():
        give(mine).wait_send()

    @pl.when(leads)
    def _():
        def sent(buffer, sem):
            landed(buffer, buffer, sem, far_recv.at[0]).wait_send()

        if near > 1:
            sent(asked.at[pl.ds(0, near - 1)], near_send)
        if far > 1:
            sent(req_in.at[pl.ds(0, (far - 1) * near)], far_send)
        for member in range(leader):
            sent(res_out, res_send.at[member])
        if tiles > 1:
            sent(res_out.at[pl.ds(0, tiles - 1)], res_send.at[leader])


def scoped(tiles, groups, near, cap, packs, *refs):
    dma = pltpu.SemaphoreType.DMA
    one, chunks = dma(()), tiles // max(near, LANES // cap)
    pl.run_scoped(
        functools.partial(kernel, tiles, groups, near, cap, packs, *refs),
        pltpu.SemaphoreType.REGULAR(()), dma((max(1, groups - 1),)), one, dma((tiles // near,)), dma((chunks,)),
        dma((7,)), one, one, one, dma((groups,)),
    )


def on_device(ensemble, control, vert_loc, obs_source, obs_column, obs_slot, obs_frac, obs_count):
    tiles, groups = lax.axis_size("tile"), lax.axis_size("member")
    members, slots, levels, cols = ensemble.shape
    obs = obs_column.shape[0]
    cap = max(4, 2 * obs // tiles)
    near = max(d for d in range(1, tiles + 1) if tiles % d == 0 and d * d <= tiles)
    packs = max(1, min(LANES // cap, levels // 8))
    rows = levels // packs
    vmem = pl.BlockSpec(memory_space=pltpu.VMEM)
    hbm = pl.BlockSpec(memory_space=pl.ANY)
    return pl.pallas_call(
        functools.partial(scoped, tiles, groups, near, cap, packs),
        out_shape=pltpu.VMEM((levels, obs), F32),
        in_specs=[hbm] * 7 + [pl.BlockSpec(memory_space=pltpu.SMEM)],
        out_specs=vmem,
        scratch_shapes=[
            pltpu.VMEM((levels, levels), BF16),
            pltpu.VMEM((1, obs), jnp.int32),
            pltpu.VMEM((1, obs), jnp.int32),
            pltpu.VMEM((1, obs), jnp.int32),
            pltpu.VMEM((1, obs), F32),
            pltpu.VMEM((members, slots, levels, cols), BF16),
            pltpu.VMEM((members * levels, cols), BF16),
            pltpu.VMEM((members * levels, cols), F32),
            pltpu.VMEM((slots * levels, cols), F32),
            pltpu.VMEM((max(1, groups - 1), slots * levels, cols), F32),
            pltpu.VMEM((near, tiles // near, 2, LANES), F32),
            pltpu.VMEM((near, tiles // near, 2, LANES), F32),
            pltpu.VMEM((tiles, 2, LANES), F32),
            pltpu.VMEM((tiles, rows, LANES), F32),
            pltpu.VMEM((tiles, rows, LANES), F32),
            pltpu.VMEM((tiles * cap, obs), BF16),
        ],
        compiler_params=pltpu.CompilerParams(collective_id=0, has_side_effects=True),
    )(
        ensemble,
        control.reshape(members * levels, cols),
        vert_loc,
        obs_source.reshape(1, obs),
        obs_column.reshape(1, obs),
        obs_slot.reshape(1, obs),
        obs_frac.reshape(1, obs),
        obs_count,
    )


def solution(mesh):
    placed = (
        P("member", None, None, "tile"),
        P("member", None, "tile"),
        P(),
        P("tile", None),
        P("tile"),
        P("tile"),
        P("tile"),
        P("tile"),
    )
    return jax.shard_map(
        on_device, mesh=mesh, in_specs=placed, out_specs=P(None, "tile"), check_vma=False
    )
```

```python
import functools

import jax
import jax.numpy as jnp
from jax import lax
from jax.experimental import pallas as pl
from jax.experimental.pallas import tpu as pltpu
from jax.sharding import PartitionSpec as P

MESH = pl.DeviceIdType.MESH
LANES = 128
F32 = jnp.float32
BF16 = jnp.bfloat16


def iota(shape, axis):
    return lax.broadcasted_iota(jnp.int32, shape, axis)


def one_hot(condition):
    return jnp.where(condition, F32(1.0), F32(0.0)).astype(BF16)


def dot(a, b):
    return jnp.dot(a, b, preferred_element_type=F32)


def dot_nt(a, b):
    return lax.dot_general(a, b, (((1,), (1,)), ((), ())), preferred_element_type=F32)


def two_pieces(x):
    high = x.astype(BF16)
    return high, (x - high.astype(F32)).astype(BF16)


def turned(x, shift):
    shift = shift % LANES
    return x if shift == 0 else pltpu.roll(x, shift, 1)


def kernel(
    tiles, groups, near, cap, packs,
    ens_hbm, ctl_hbm, vloc_hbm, source_hbm, column_hbm, slot_hbm, frac_hbm, count_ref,
    out_ref,
    vloc_ref, source_ref, column_ref, slot_ref, frac_ref, ens, ctl, weighted, part, part_in, asked, relay, req_in, res_out, res_in, place,
    rest_in, part_recv, near_recv, far_recv, res_recv,
    load_sem, part_send, near_send, far_send, res_send,
):
    me = lax.axis_index("tile")
    mine = lax.axis_index("member")
    leader = groups - 1
    collector = leader - 1
    leads = mine == leader
    members, slots, levels, cols = ens.shape
    rows = levels // packs
    obs = column_ref.shape[1]
    owners = LANES // cap
    far = tiles // near
    low, high = lax.rem(me, near), me // near
    chunk = max(near, owners)
    chunks = tiles // chunk
    lines = chunk // near
    spans = chunk // owners
    width = spans * LANES

    def loaded(index, source, target):
        return pltpu.make_async_copy(source, target, load_sem.at[index])

    loads = [
        loaded(0, source_hbm, source_ref), loaded(1, column_hbm, column_ref),
        loaded(2, slot_hbm, slot_ref), loaded(3, frac_hbm, frac_ref),
        loaded(4, vloc_hbm, vloc_ref), loaded(5, ctl_hbm, ctl), loaded(6, ens_hbm, ens),
    ]

    def near_peer(step):
        return lax.rem(low + step, near)

    def far_peer(step):
        return lax.rem(high + step, far)

    barrier = pltpu.get_barrier_semaphore()

    def greet(tile, member):
        pl.semaphore_signal(
            barrier, inc=1, device_id={"tile": tile, "member": member}, device_id_type=MESH
        )

    def taker(digit, direct):
        return jnp.where((digit == 0) == direct, leader, collector)

    @pl.when(leads)
    def _():
        for step in range(1, near):
            greet(high * near + near_peer(step), taker(near_peer(step), True))
        for step in range(1, far):
            greet(far_peer(step) * near + low, taker(low, False))
        for member in range(leader):
            greet(me, member)

    @pl.when(jnp.logical_not(leads) & ((mine != collector) | (low == 0)))
    def _():
        greet(me, taker(low, True))

    for load in loads:
        load.start()

    def near_copy(peer, line):
        return pltpu.make_async_remote_copy(
            src_ref=asked.at[peer], dst_ref=relay.at[line],
            send_sem=near_send, recv_sem=near_recv,
            device_id={"tile": high * near + peer, "member": leader}, device_id_type=MESH,
        )

    def ranked():
        source = source_ref[...]
        hits = source == iota((tiles, obs), 0)
        hits_f = jnp.where(hits, F32(1.0), F32(0.0))
        before = one_hot(iota((LANES, LANES), 0) < iota((LANES, LANES), 1))
        seen = jnp.zeros((tiles, 1), F32)
        ranks = []
        for block in range(obs // LANES):
            hit = hits_f[:, block * LANES:(block + 1) * LANES]
            ahead = dot(hit.astype(BF16), before) + seen
            ranks.append(jnp.sum(ahead * hit, axis=0, keepdims=True))
            seen = seen + jnp.sum(hit, axis=1, keepdims=True)
        rank = jnp.concatenate(ranks, axis=1).astype(jnp.int32)
        return source, hits, rank

    def placed(source, rank):
        live = iota((1, obs), 1) < count_ref[0]
        position = jnp.where(live, source * cap + rank, -1)
        return one_hot(position == iota((tiles * cap, obs), 0))

    for load in loads[:4]:
        load.wait()

    @pl.when(leads)
    def _():
        source, hits, rank = ranked()
        spread = one_hot(rank == lax.rem(iota((LANES, obs), 0), cap))
        frac = frac_ref[...]
        frac_0 = frac.astype(BF16).astype(F32)
        frac_1 = (frac - frac_0).astype(BF16).astype(F32)
        frac_2 = frac - frac_0 - frac_1
        values = [column_ref[...].astype(F32), slot_ref[...].astype(F32), frac_0, frac_1, frac_2]
        packed = dot_nt(
            jnp.concatenate([jnp.where(hits, v, F32(0.0)) for v in values], axis=0).astype(BF16), spread
        )
        packed = [packed[i * tiles:(i + 1) * tiles] for i in range(len(values))]
        seat = iota((tiles, LANES), 1) // cap == lax.rem(me, owners)
        code = jnp.where(seat, packed[0] + cols * packed[1], F32(0.0))
        part_of = jnp.where(seat, packed[2] + packed[3] + packed[4], F32(0.0))
        for tile in range(tiles):
            asked[tile % near, tile // near, 0:1] = code[tile:tile + 1]
            asked[tile % near, tile // near, 1:2] = part_of[tile:tile + 1]

        @pl.when(low == 0)
        def _():
            pl.semaphore_wait(barrier, near + groups - 2)

        @pl.when(low != 0)
        def _():
            pl.semaphore_wait(rest_in, 1)

        for step in range(near - 1, 0, -1):
            near_copy(near_peer(step), low).start()
        relay[low] = asked[low]
        place[...] = placed(source, rank)

    def entered(count):
        pl.semaphore_wait(barrier, count)
        pl.semaphore_signal(
            rest_in, inc=1, device_id={"tile": me, "member": leader}, device_id_type=MESH
        )

    @pl.when((mine == collector) & (low != 0))
    def _():
        entered(near + groups - 2)

    batch = max(d for d in range(1, max(1, LANES // levels) + 1) if members % d == 0)
    wide = batch * levels
    repeat = one_hot(lax.rem(iota((wide, levels), 0), levels) == iota((wide, levels), 1))
    for load in loads[4:6]:
        load.wait()
    tall = dot(repeat, vloc_ref[...]).astype(BF16)
    full = dot_nt(tall, repeat)
    factor = jnp.where(
        iota((wide, wide), 0) // levels == iota((wide, wide), 1) // levels, full, F32(0.0)
    ).astype(BF16)
    for step in range(members // batch):
        weighted[step * wide:(step + 1) * wide] = dot(factor, ctl[step * wide:(step + 1) * wide])

    loads[6].wait()
    for slot in range(slots):
        total = jnp.zeros((levels, cols), F32)
        for k in range(members):
            total = total + ens[k, slot].astype(F32) * weighted[k * levels:(k + 1) * levels]
        part[slot * levels:(slot + 1) * levels] = total

    def give(member):
        return pltpu.make_async_remote_copy(
            src_ref=part, dst_ref=part_in.at[member],
            send_sem=part_send, recv_sem=part_recv.at[member],
            device_id={"tile": me, "member": leader}, device_id_type=MESH,
        )

    @pl.when(jnp.logical_not(leads))
    def _():
        @pl.when((mine == collector) & (low == 0))
        def _():
            entered(far)

        @pl.when(mine != collector)
        def _():
            pl.semaphore_wait(barrier, 1)

        give(mine).start()
        source, _, rank = ranked()
        place[...] = placed(source, rank)

    lane = iota((1, LANES), 1)
    stride = jnp.where(2 * me < tiles, 1, chunks - 1)
    home = me // chunk

    def chunk_at(step):
        return lax.rem(home + stride * step, chunks)

    def served(step):
        return home if step == 0 else jnp.where(step - 1 < home, step - 1, step)

    def unless(step, condition, body):
        if step == 0:
            pl.when(condition)(body)
        else:
            body()

    def reply_to(tile, member):
        return pltpu.make_async_remote_copy(
            src_ref=res_out.at[tile], dst_ref=res_in.at[me],
            send_sem=res_send.at[member], recv_sem=res_recv.at[home],
            device_id={"tile": tile, "member": member}, device_id_type=MESH,
        )

    def landed(source, target, send, recv):
        return pltpu.make_async_remote_copy(
            src_ref=source, dst_ref=target, send_sem=send, recv_sem=recv,
            device_id={"tile": me, "member": leader}, device_id_type=MESH,
        )

    @pl.when(leads)
    def _():
        def far_copy(peer, line):
            return pltpu.make_async_remote_copy(
                src_ref=relay.at[:, peer], dst_ref=req_in.at[pl.ds(line * near, near)],
                send_sem=far_send, recv_sem=far_recv.at[line],
                device_id={"tile": peer * near + low, "member": leader}, device_id_type=MESH,
            )

        if near > 1:
            others = relay.at[pl.ds(0, near - 1)]
            landed(others, others, near_send, near_recv).wait_recv()

        @pl.when(low == 0)
        def _():
            pl.semaphore_wait(rest_in, 1)

        @pl.when(low != 0)
        def _():
            pl.semaphore_wait(barrier, far - 1)

        for step in range(far - 1, 0, -1):
            far_copy(far_peer(step), high).start()
        req_in[pl.ds(high * near, near)] = relay[:, high]

        increment = part[...]
        for member in range(leader):
            give(member).wait_recv()
            increment = increment + part_in[member]
        pieces = jnp.concatenate(two_pieces(increment), axis=1)

        for step in range(chunks):
            group = served(step)
            for i in range(lines):
                line = group * lines + i
                unless(step, line != high, lambda line=line: far_copy(line, line).wait_recv())
            answers = []
            for s in range(spans):
                first = group * chunk + s * owners
                code, frac = req_in[first, 0:1], req_in[first, 1:2]
                for i in range(1, owners):
                    code = code + req_in[first + i, 0:1]
                    frac = frac + req_in[first + i, 1:2]
                wanted = jnp.floor((code + 0.5) * (1.0 / cols))
                column = (code - cols * wanted).astype(jnp.int32)
                pick = one_hot(iota((cols, LANES), 0) == column)
                pick = jnp.concatenate([pick, pick], axis=0)
                half = (slots + 1) // 2 * levels
                columns = jnp.concatenate([dot(pieces[:half], pick), dot(pieces[half:], pick)], axis=0)
                answer = jnp.zeros((levels, LANES), F32)
                for slot in range(slots):
                    weight = jnp.where(
                        wanted == slot, 1.0 - frac, jnp.where(wanted == slot - 1, frac, F32(0.0))
                    )
                    answer = answer + weight * columns[slot * levels:(slot + 1) * levels]
                answers.append(answer)
            for t in range(chunk):
                s, i = t // owners, t % owners
                tile = group * chunk + t
                packet = jnp.zeros((rows, LANES), F32)
                for j in range(packs):
                    block = answers[s][j * rows:(j + 1) * rows]
                    packet = jnp.where(lane // cap == j, turned(block, (j - i) * cap), packet)
                res_out[tile] = packet
                if step == 0:
                    @pl.when(tile == me)
                    def _():
                        res_in[me] = packet
                for member in range(leader):
                    reply_to(tile, member).start()
            for t in range(chunk):
                tile = group * chunk + t
                unless(step, tile != me, lambda tile=tile: reply_to(tile, leader).start())

    both = jnp.zeros((2 * levels, obs), F32)
    for step in range(chunks):
        group = chunk_at(step)
        whole = res_in.at[pl.ds(group * chunk, chunk)]
        if step == 0:
            if chunk > 1:
                @pl.when(leads)
                def _():
                    rest = res_in.at[pl.ds(0, chunk - 1)]
                    landed(rest, rest, res_send.at[leader], res_recv.at[group]).wait_recv()

            @pl.when(jnp.logical_not(leads))
            def _():
                landed(whole, whole, res_send.at[leader], res_recv.at[group]).wait_recv()
        else:
            landed(whole, whole, res_send.at[leader], res_recv.at[group]).wait_recv()
        columns = []
        for s in range(spans):
            bands = [jnp.zeros((rows, LANES), F32)] * packs
            for i in range(owners):
                got = res_in[group * chunk + s * owners + i]
                for j in range(packs):
                    bands[j] = jnp.where(lane // cap == i, turned(got, (i - j) * cap), bands[j])
            columns.append(jnp.concatenate(bands, axis=0))
        upper, lower = two_pieces(jnp.concatenate(columns, axis=1))
        first = pl.multiple_of(group * width, LANES)
        both = both + dot(jnp.concatenate([upper, lower], axis=0), place[pl.ds(first, width)])
    out_ref[...] = both[:levels] + both[levels:]

    @pl.when(jnp.logical_not(leads))
    def _():
        give(mine).wait_send()

    @pl.when(leads)
    def _():
        def sent(buffer, sem):
            landed(buffer, buffer, sem, far_recv.at[0]).wait_send()

        if near > 1:
            sent(asked.at[pl.ds(0, near - 1)], near_send)
        if far > 1:
            sent(req_in.at[pl.ds(0, (far - 1) * near)], far_send)
        for member in range(leader):
            sent(res_out, res_send.at[member])
        if tiles > 1:
            sent(res_out.at[pl.ds(0, tiles - 1)], res_send.at[leader])


def scoped(tiles, groups, near, cap, packs, *refs):
    dma = pltpu.SemaphoreType.DMA
    one, chunks = dma(()), tiles // max(near, LANES // cap)
    pl.run_scoped(
        functools.partial(kernel, tiles, groups, near, cap, packs, *refs),
        pltpu.SemaphoreType.REGULAR(()), dma((max(1, groups - 1),)), one, dma((tiles // near,)), dma((chunks,)),
        dma((7,)), one, one, one, dma((groups,)),
    )


def on_device(ensemble, control, vert_loc, obs_source, obs_column, obs_slot, obs_frac, obs_count):
    tiles, groups = lax.axis_size("tile"), lax.axis_size("member")
    members, slots, levels, cols = ensemble.shape
    obs = obs_column.shape[0]
    cap = max(4, 2 * obs // tiles)
    near = max(d for d in range(1, tiles + 1) if tiles % d == 0 and d * d <= tiles)
    packs = max(1, min(LANES // cap, levels // 8))
    rows = levels // packs
    vmem = pl.BlockSpec(memory_space=pltpu.VMEM)
    hbm = pl.BlockSpec(memory_space=pl.ANY)
    return pl.pallas_call(
        functools.partial(scoped, tiles, groups, near, cap, packs),
        out_shape=pltpu.VMEM((levels, obs), F32),
        in_specs=[hbm] * 7 + [pl.BlockSpec(memory_space=pltpu.SMEM)],
        out_specs=vmem,
        scratch_shapes=[
            pltpu.VMEM((levels, levels), BF16),
            pltpu.VMEM((1, obs), jnp.int32),
            pltpu.VMEM((1, obs), jnp.int32),
            pltpu.VMEM((1, obs), jnp.int32),
            pltpu.VMEM((1, obs), F32),
            pltpu.VMEM((members, slots, levels, cols), BF16),
            pltpu.VMEM((members * levels, cols), BF16),
            pltpu.VMEM((members * levels, cols), F32),
            pltpu.VMEM((slots * levels, cols), F32),
            pltpu.VMEM((max(1, groups - 1), slots * levels, cols), F32),
            pltpu.VMEM((near, tiles // near, 2, LANES), F32),
            pltpu.VMEM((near, tiles // near, 2, LANES), F32),
            pltpu.VMEM((tiles, 2, LANES), F32),
            pltpu.VMEM((tiles, rows, LANES), F32),
            pltpu.VMEM((tiles, rows, LANES), F32),
            pltpu.VMEM((tiles * cap, obs), BF16),
        ],
        compiler_params=pltpu.CompilerParams(collective_id=0, has_side_effects=True),
    )(
        ensemble,
        control.reshape(members * levels, cols),
        vert_loc,
        obs_source.reshape(1, obs),
        obs_column.reshape(1, obs),
        obs_slot.reshape(1, obs),
        obs_frac.reshape(1, obs),
        obs_count,
    )


def solution(mesh):
    placed = (
        P("member", None, None, "tile"),
        P("member", None, "tile"),
        P(),
        P("tile", None),
        P("tile"),
        P("tile"),
        P("tile"),
        P("tile"),
    )
    return jax.shard_map(
        on_device, mesh=mesh, in_specs=placed, out_specs=P(None, "tile"), check_vma=False
    )
```
